256 devices in a mesh: region: 2 (over z), member: 16 (over y, core), space: 8 (over x).
Axes of the slice: x: 8, y: 8, z: 2, core: 2. Of those that a mesh axis runs over, the one named last changes fastest.
The devices are a block of a 8x8x16 slice.
Arguments:
- prior_trials: bfloat16 [80, 12288, 256], P('member', ('region', 'space')), parts along dimension 1, may hold values from -6 to 6
- prior_at_sensors: bfloat16 [80, 12288], P('member', ('region', 'space')), parts along dimension 1, may hold values from -6 to 6
- sensor_readings: bfloat16 [12288], P(('region', 'space')), parts along dimension 0, may hold values from -8 to 8
- sensor_noise_spread: bfloat16 [12288], P(('region', 'space')), parts along dimension 0, may hold values from 1 to 10
- nearby_readings: int32 [12288, 128], P(('region', 'space')), parts along dimension 0, may hold values from 0 to 1407, as said below
- subarea_cutoff_level: int32 [12288], P(('region', 'space')), parts along dimension 0, may hold values from 0 to 3
Outputs:
- analysis: bfloat16 [80, 12288, 256], P('member', ('region', 'space')), parts along dimension 1
The draws below stay inside these ranges and needn't reach their ends.
There are 2 independent parts, one for each index of `region`. The reference program is written for one: setup_inputs(seed, part) draws one part's arguments, and reference() takes and returns one part's arrays. A program takes and returns all parts, laid end to end along the dimension named above; each array names one. Nothing has to cross between parts.
Inputs may be any that keep to these rules, and one draw needn't show every extreme that they name: `nearby_readings`: row c lists 128 distinct observations whose region-wide index o lies within (subarea_cutoff_level[c] + 2) * 64 of c and inside the region.
All inputs are finite; a program needn't handle non-finite values. Where the reference program divides by a largest or mean magnitude, that divisor is 1e-20 or more.
Results may differ from the reference program's by a relative error of at most 0.0053.
Values may be sent and summed in bfloat16 or wider, within the bound.
No kernel may reach another device: no remote copies, remote signals or barrier semaphores. Data moves between devices by JAX's collectives and lax.ppermute only.
A program may use at most 64 MiB of HBM per device.

```python
import math
import jax
import jax.numpy as jnp
from jax import lax

TRIAL_COUNT = 80
CELL_QUANTITIES = 256
OBS_DOM = 128
TIERS = 4
NS_STEPS = 4
PATCH_CELLS = 768
AREA_CELLS = 6144
HALO = 320


def tier_table(key):
    return jax.random.randint(jax.random.fold_in(key, 11), (AREA_CELLS,), 0, TIERS).astype(jnp.int32)


def draw_subarea_cutoff_level(key, part):
    return tier_table(key)


def draw_nearby_readings(key, part):
    tier_ids = tier_table(key)
    columns = jnp.arange(AREA_CELLS, dtype=jnp.int32)
    width_all = 2 * HALO + 1
    offsets = jnp.arange(width_all, dtype=jnp.int32) - HALO
    reach_twice = (tier_ids + 2) * OBS_DOM
    position = columns[:, None] + offsets[None, :]
    usable = (2 * jnp.abs(offsets)[None, :] <= reach_twice[:, None]) & (position >= 0) & (position < AREA_CELLS)
    raw_bits = jax.random.randint(jax.random.fold_in(key, 12), (AREA_CELLS, width_all), 0, 1 << 20).astype(jnp.int32)
    slot_ids = (offsets + HALO)[None, :]
    score = jnp.where(usable, raw_bits * width_all + slot_ids, -1 - slot_ids)
    unused, chosen = lax.top_k(score, OBS_DOM)
    return ((columns % PATCH_CELLS)[:, None] + chosen).astype(jnp.int32)


def draw_sensor_readings(key, part):
    ramp = jnp.arange(AREA_CELLS, dtype=jnp.float32) / AREA_CELLS
    noise = jnp.clip(jax.random.normal(jax.random.fold_in(key, 22), (AREA_CELLS,), jnp.float32), -4.0, 4.0)
    values = 0.6 * (1.0 + 2.0 * ramp) * noise
    return values.astype(jnp.bfloat16)


def block_levels(key, extent, split, low, largest):
    level, own = 1.0, jax.random.fold_in(key, 6)
    for dim, parts in split:
        heights = jnp.exp(jax.random.uniform(jax.random.fold_in(own, dim), (parts,), jnp.float32, low / len(split), largest / len(split)))
        level = level * jnp.repeat(heights, extent[dim] // parts).reshape([-1 if axis == dim else 1 for axis in range(len(extent))])
    return level


def gaussian(own_key, shape, scale, most, pieces=(), kind=jnp.bfloat16):
    drawn = scale * jax.random.normal(own_key, shape, jnp.float32)
    if pieces:
        drawn = drawn * block_levels(own_key, shape, pieces, -0.22, 0.18)
    return jnp.clip(drawn, -most, most).astype(kind)


def setup_inputs(seed: int = 0, part: int = 0) -> dict:
    keys = jax.random.split(jax.random.key(seed), 7)
    own_keys = jax.random.split(jax.random.fold_in(keys[6], part), 7)
    return {
        "prior_trials": gaussian(own_keys[0], (TRIAL_COUNT, AREA_CELLS, CELL_QUANTITIES), 1.0, 6.0, ((0, 16), (1, 8))),
        "prior_at_sensors": gaussian(own_keys[1], (TRIAL_COUNT, AREA_CELLS), 1.0, 6.0, ((0, 16), (1, 8))),
        "sensor_readings": draw_sensor_readings(jax.random.fold_in(jax.random.fold_in(keys[6], part), 71), part),
        "sensor_noise_spread": jnp.clip(jnp.exp(math.log(10.0) - 2.3025851 * jax.random.uniform(own_keys[3], (AREA_CELLS,), jnp.float32) ** block_levels(own_keys[3], (AREA_CELLS,), ((0, 8),), -0.2, 0.2)), 1.0, 10.0).astype(jnp.bfloat16),
        "nearby_readings": draw_nearby_readings(jax.random.fold_in(jax.random.fold_in(keys[6], part), 71), part),
        "subarea_cutoff_level": draw_subarea_cutoff_level(jax.random.fold_in(jax.random.fold_in(keys[6], part), 71), part),
    }


def prepare(picked, trial_lines, offsets, tier_ids, obs_count):
    observ = picked[:trial_lines]
    ens_mean = lax.optimization_barrier(jnp.mean(observ, axis=0))
    anomaly = observ - ens_mean
    innovation = picked[trial_lines] - ens_mean
    radius = (tier_ids.astype(jnp.float32) + 2.0) * (0.5 * obs_count)
    distance = jnp.abs(offsets).astype(jnp.float32) / radius[:, None]
    weight = jnp.exp(-2.0 * distance * distance) / picked[trial_lines + 1]
    return (anomaly, innovation, weight)

def spread_terms(anomaly, innovation, weight, trial_lines):
    fit_sum = jnp.sum(weight * innovation * innovation)
    spread = jnp.sum(weight * lax.optimization_barrier(jnp.sum(anomaly * anomaly, axis=0))) / (trial_lines - 1.0)
    return (fit_sum, spread)

def transform(anomaly, innovation, weight, inflation, trial_lines, sweeps):
    exact = lax.Precision.HIGHEST
    weighted = anomaly * weight[None]
    gram = jnp.einsum('ank,bnk->abn', weighted, anomaly, precision=exact)
    identity = jnp.eye(trial_lines, dtype=jnp.float32)[:, :, None]
    matrix = gram + (trial_lines - 1.0) / inflation * identity
    row_bound = lax.optimization_barrier(jnp.max(lax.optimization_barrier(jnp.sum(jnp.abs(matrix), axis=1)), axis=0))
    root_iter = matrix / row_bound
    inverse = jnp.broadcast_to(identity, matrix.shape)
    for repeat in range(sweeps):
        factor = 1.5 * identity - 0.5 * jnp.einsum('abn,bcn->acn', inverse, root_iter, precision=exact)
        root_iter = jnp.einsum('abn,bcn->acn', root_iter, factor, precision=exact)
        inverse = jnp.einsum('abn,bcn->acn', factor, inverse, precision=exact)
    inv_root = inverse / jnp.sqrt(row_bound)
    target = lax.optimization_barrier(jnp.sum(weighted * innovation[None], axis=2))
    half_gain = jnp.einsum('abn,bn->an', inv_root, target, precision=exact)
    mean_gain = jnp.einsum('abn,bn->an', inv_root, half_gain, precision=exact)
    weights_full = jnp.sqrt(trial_lines - 1.0) * inv_root + mean_gain[:, None, :]
    centred = weights_full - lax.optimization_barrier(jnp.mean(weights_full, axis=0, keepdims=True)) + 1.0 / trial_lines
    return centred.astype(jnp.bfloat16)

def reference(prior_trials, prior_at_sensors, sensor_readings, sensor_noise_spread, nearby_readings, subarea_cutoff_level):
    trial_lines = prior_at_sensors.shape[0]
    obs_count = nearby_readings.shape[1]
    columns = jnp.arange(AREA_CELLS, dtype=jnp.int32)
    global_obs = (nearby_readings + (columns // PATCH_CELLS * PATCH_CELLS - HALO)[:, None]).astype(jnp.int32)
    block_count = AREA_CELLS // PATCH_CELLS

    def block_data(block_no):
        patch_start_index = (block_no * PATCH_CELLS).astype(jnp.int32)
        obs_lists = lax.dynamic_slice_in_dim(global_obs, patch_start_index, PATCH_CELLS, 0)
        col_ids = lax.dynamic_slice_in_dim(columns, patch_start_index, PATCH_CELLS, 0)
        tier_ids = lax.dynamic_slice_in_dim(subarea_cutoff_level, patch_start_index, PATCH_CELLS, 0)
        ens_part = jnp.take(prior_at_sensors, obs_lists, axis=1).astype(jnp.float32)
        value_part = jnp.take(sensor_readings, obs_lists).astype(jnp.float32)[None]
        error_part = jnp.take(sensor_noise_spread, obs_lists).astype(jnp.float32)[None]
        picked = jnp.concatenate([ens_part, value_part, error_part], axis=0)
        return prepare(picked, trial_lines, obs_lists - col_ids[:, None], tier_ids, obs_count)

    def block_sums(block_no):
        anomaly, innovation, weight = block_data(block_no)
        return spread_terms(anomaly, innovation, weight, trial_lines)
    fits, spreads = lax.map(block_sums, jnp.arange(block_count, dtype=jnp.int32))
    inflation = jnp.sum(fits) / jnp.sum(spreads)

    def block_analysis(block_no):
        anomaly, innovation, weight = block_data(block_no)
        trans_w = transform(anomaly, innovation, weight, inflation, trial_lines, NS_STEPS)
        trans_w = lax.optimization_barrier(trans_w).astype(jnp.float32)
        patch_start_index = (block_no * PATCH_CELLS).astype(jnp.int32)
        quantity_lines = lax.dynamic_slice_in_dim(prior_trials, patch_start_index, PATCH_CELLS, 1).astype(jnp.float32)
        updated = jnp.einsum('inc,ijn->jnc', quantity_lines, trans_w, precision=lax.Precision.HIGHEST)
        return updated.astype(jnp.bfloat16)
    piled_pieces = lax.map(block_analysis, jnp.arange(block_count, dtype=jnp.int32))
    return jnp.transpose(piled_pieces, (1, 0, 2, 3)).reshape(trial_lines, AREA_CELLS, prior_trials.shape[2])
```

```python
import jax
import jax.numpy as jnp
from jax import lax
from jax.experimental import pallas as pl
from jax.experimental.pallas import tpu as pltpu
from jax.sharding import Mesh
from jax.sharding import PartitionSpec as P

NS_STEPS = 4
MEMBER = ("member_0", "member_1")
LANES = 128
SUB = 8


def spread_copies(value, axis):
    copies = jnp.broadcast_to(value, (lax.axis_size(axis), *value.shape))
    return lax.all_to_all(copies, axis, split_axis=0, concat_axis=0, tiled=True)


def with_halo(value, axis, width):
    count, length = lax.axis_size(axis), value.shape[1]
    up = [(i, i + 1) for i in range(count - 1)]
    down = [(j, i) for i, j in up]
    before = lax.ppermute(value[:, length - width :], axis, up)
    after = lax.ppermute(value[:, :width], axis, down)
    return jnp.concatenate([before, value, after], axis=1)


def lookup(table_rows, low, high):
    tiles = 6
    found = jnp.take_along_axis(table_rows(0), low, axis=1, mode="promise_in_bounds")
    for t in range(1, tiles):
        value = jnp.take_along_axis(table_rows(t), low, axis=1, mode="promise_in_bounds")
        found = jnp.where(high == t, value, found)
    return found


def make_table_kernel(members, halo):
    def kernel(first_ref, window_ref, lists_ref, tiers_ref, anom_ref, innov_ref, weight_ref, sums_ref, table, flat):
        tiles = window_ref.shape[0]
        for t in range(tiles):
            raw = window_ref[t].astype(jnp.float32)
            observ = raw[:members]
            mean = jnp.sum(observ, axis=0, keepdims=True) * (1.0 / members)
            anomaly = observ - mean
            innov = raw[members : members + 1] - mean
            noise = raw[members + 1 : members + 2]
            table[t, :members] = anomaly
            table[t, members : members + 1] = innov
            table[t, members + 1 : members + 2] = noise
            energy = jnp.sum(anomaly * anomaly, axis=0, keepdims=True)
            flat[t, 0:SUB] = jnp.broadcast_to(innov * innov / noise, (SUB, LANES))
            flat[t, SUB : 2 * SUB] = jnp.broadcast_to(energy / noise, (SUB, LANES))

        columns = lists_ref.shape[0]

        def decay_of(index, start, tiers):
            column = start + lax.broadcasted_iota(jnp.int32, (SUB, LANES), 0)
            radius = (tiers.astype(jnp.float32) + 2.0) * (0.5 * LANES)
            distance = jnp.abs(index - halo - column).astype(jnp.float32) / radius
            return jnp.exp(-2.0 * distance * distance)

        def block_sum(i, carry):
            fit, spread = carry
            start = pl.multiple_of(i * SUB, SUB)
            index = lists_ref[pl.ds(start, SUB), :]
            first_tile = start // LANES
            local = index - first_tile * LANES
            low, high = local & (LANES - 1), local >> 7
            decay = decay_of(index, start, tiers_ref[pl.ds(start, SUB), :])
            fits = lookup(lambda t: flat[first_tile + t, 0:SUB], low, high)
            spreads = lookup(lambda t: flat[first_tile + t, SUB : 2 * SUB], low, high)
            return fit + decay * fits, spread + decay * spreads

        zero = jnp.zeros((SUB, LANES), jnp.float32)
        fit, spread = lax.fori_loop(0, columns // SUB, block_sum, (zero, zero))
        sums_ref[0:1, :] = jnp.broadcast_to(jnp.sum(fit), (1, LANES))
        sums_ref[1:2, :] = jnp.broadcast_to(jnp.sum(spread), (1, LANES))

        first = first_ref[0]
        own = innov_ref.shape[0]
        groups = members // SUB

        def own_block(b, unused):
            start = pl.multiple_of(first + b * SUB, SUB)
            indices = lists_ref[pl.ds(start, SUB), :]
            decay = decay_of(indices, start, tiers_ref[pl.ds(start, SUB), :])
            innovs, noises = [], []
            for s in range(SUB):
                column = start + s
                first_tile = column // LANES
                local = jnp.broadcast_to(indices[s : s + 1], (SUB, LANES)) - first_tile * LANES
                low, high = local & (LANES - 1), local >> 7
                for g in range(groups):
                    anom_ref[b * SUB + s, g * SUB : (g + 1) * SUB] = lookup(
                        lambda t: table[first_tile + t, g * SUB : (g + 1) * SUB], low, high
                    )
                tail = lookup(lambda t: table[first_tile + t, members : members + SUB], low, high)
                innovs.append(tail[0:1])
                noises.append(tail[1:2])
            rows = pl.ds(pl.multiple_of(b * SUB, SUB), SUB)
            innov_ref[rows, :] = jnp.concatenate(innovs, axis=0)
            weight_ref[rows, :] = decay / jnp.concatenate(noises, axis=0)
            return unused

        lax.fori_loop(0, own // SUB, own_block, 0)

    return kernel


def select_domains(window, first, lists, tiers, members, own, halo):
    obs = lists.shape[1]
    tiles = window.shape[0]
    f32 = jnp.float32
    return pl.pallas_call(
        make_table_kernel(members, halo),
        in_specs=[
            pl.BlockSpec(memory_space=pltpu.SMEM),
            pl.BlockSpec(memory_space=pltpu.VMEM),
            pl.BlockSpec(memory_space=pltpu.VMEM),
            pl.BlockSpec(memory_space=pltpu.VMEM),
        ],
        out_specs=[pl.BlockSpec(memory_space=pltpu.VMEM)] * 4,
        out_shape=[
            jax.ShapeDtypeStruct((own, members, obs), f32),
            jax.ShapeDtypeStruct((own, obs), f32),
            jax.ShapeDtypeStruct((own, obs), f32),
            jax.ShapeDtypeStruct((2, LANES), f32),
        ],
        scratch_shapes=[
            pltpu.VMEM((tiles, members + SUB, LANES), f32),
            pltpu.VMEM((tiles, 2 * SUB, LANES), f32),
        ],
        name="select_domains",
    )(first, window, lists, tiers)


def transform(anomaly, innovation, weight, inflation, sweeps):
    exact = lax.Precision.HIGH
    trial_lines = anomaly.shape[1]
    weighted = anomaly * weight[:, None]
    gram = jnp.einsum("nak,nbk->nab", weighted, anomaly, precision=exact)
    identity = jnp.eye(trial_lines, dtype=jnp.float32)[None]
    matrix = gram + (trial_lines - 1.0) / inflation * identity
    row_bound = jnp.max(jnp.sum(jnp.abs(matrix), axis=2), axis=1)[:, None, None]
    root_iter = matrix / row_bound
    inverse = jnp.broadcast_to(identity, matrix.shape)
    for repeat in range(sweeps):
        if repeat == 0:
            factor = 1.5 * identity - 0.5 * root_iter
        else:
            factor = 1.5 * identity - 0.5 * jnp.einsum("nab,nbc->nac", inverse, root_iter, precision=exact)
        if repeat < sweeps - 1:
            root_iter = jnp.einsum("nab,nbc->nac", root_iter, factor, precision=exact)
        inverse = factor if repeat == 0 else jnp.einsum("nab,nbc->nac", factor, inverse, precision=exact)
    inv_root = inverse / jnp.sqrt(row_bound)
    target = jnp.sum(weighted * innovation[:, None], axis=2)
    half_gain = jnp.einsum("nab,nb->na", inv_root, target, precision=exact)
    mean_gain = jnp.einsum("nab,nb->na", inv_root, half_gain, precision=exact)
    weights_full = jnp.sqrt(trial_lines - 1.0) * inv_root + mean_gain[:, :, None]
    centred = weights_full - jnp.mean(weights_full, axis=1, keepdims=True) + 1.0 / trial_lines
    return centred.astype(jnp.bfloat16)


def per_device(
    prior_trials,
    prior_at_sensors,
    sensor_readings,
    sensor_noise_spread,
    nearby_readings,
    subarea_cutoff_level,
):
    held, patch_cells, quantities = prior_trials.shape
    obs_count = nearby_readings.shape[1]
    halo_cells = 5 * obs_count // 2
    groups = lax.axis_size(MEMBER)
    members = held * groups
    domains = patch_cells // groups

    gathered = spread_copies(prior_at_sensors, MEMBER).reshape(members, patch_cells)
    outgoing = prior_trials.reshape(held, groups, domains, quantities).transpose(1, 0, 2, 3)
    outgoing, gathered = lax.optimization_barrier((outgoing, gathered))
    incoming = lax.all_to_all(outgoing, MEMBER, split_axis=0, concat_axis=0, tiled=True)
    incoming = incoming.reshape(members, domains, quantities)

    obs_rows = jnp.stack([sensor_readings, sensor_noise_spread], axis=0)
    window = with_halo(jnp.concatenate([gathered, obs_rows], axis=0), "space", halo_cells)
    tiles = patch_cells // LANES + 6
    window = jnp.pad(window, ((0, SUB - 2), (0, tiles * LANES - window.shape[1])))
    window = window.reshape(members + SUB, tiles, LANES).transpose(1, 0, 2)

    first = (lax.axis_index(MEMBER) * domains).astype(jnp.int32).reshape(1)
    anomaly, innovation, weight, sums = select_domains(
        window, first, nearby_readings, subarea_cutoff_level[:, None], members, domains, halo_cells
    )
    total = jnp.sum(spread_copies(sums, "space").reshape(-1, 2, LANES)[:, :, 0], axis=0)
    inflation = total[0] / (total[1] / (members - 1.0))
    trans_w = transform(anomaly, innovation, weight, inflation, NS_STEPS)

    updated = jnp.einsum(
        "inc,nij->jnc", incoming, trans_w, preferred_element_type=jnp.float32
    ).astype(jnp.bfloat16)
    returned = lax.all_to_all(
        updated.reshape(groups, held, domains, quantities), MEMBER, split_axis=0, concat_axis=0, tiled=True
    )
    return returned.transpose(1, 0, 2, 3).reshape(held, patch_cells, quantities)


def solution(mesh):
    finer = Mesh(
        mesh.devices.reshape(mesh.shape["region"], 8, 2, mesh.shape["space"]),
        ("region", "member_0", "member_1", "space"),
    )
    return jax.shard_map(
        per_device,
        mesh=finer,
        in_specs=(
            P(MEMBER, ("region", "space"), None),
            P(MEMBER, ("region", "space")),
            P(("region", "space")),
            P(("region", "space")),
            P(("region", "space"), None),
            P(("region", "space")),
        ),
        out_specs=P(MEMBER, ("region", "space"), None),
        check_vma=False,
    )
```

```python
import jax
import jax.numpy as jnp
from jax import lax
from jax.experimental import pallas as pl
from jax.experimental.pallas import tpu as pltpu
from jax.sharding import Mesh
from jax.sharding import PartitionSpec as P


MEMBER = ("member_0", "member_1")
LANES = 128
SUB = 8
SPAN = 6
BATCH = 16
f32, bf16 = jnp.float32, jnp.bfloat16
NT = (((1,), (1,)), ((), ()))


def vmem():
    return pl.BlockSpec(memory_space=pltpu.VMEM)


def smem():
    return pl.BlockSpec(memory_space=pltpu.SMEM)


def spread_copies(value, axis):
    copies = jnp.broadcast_to(value, (lax.axis_size(axis), *value.shape))
    return lax.all_to_all(copies, axis, split_axis=0, concat_axis=0, tiled=True)


def shifted(value, axis, step):
    count = lax.axis_size(axis)
    return lax.ppermute(value, axis, [(i, (i + step) % count) for i in range(count)])


def with_halo(value, axis, width):
    count, length = lax.axis_size(axis), value.shape[1]
    up = [(i, i + 1) for i in range(count - 1)]
    down = [(j, i) for i, j in up]
    before = lax.ppermute(value[:, length - width :], axis, up)
    after = lax.ppermute(value[:, :width], axis, down)
    return jnp.concatenate([before, value, after], axis=1)


def decay_of(index, start, tiers, halo):
    column = start + lax.broadcasted_iota(jnp.int32, index.shape, 0)
    radius = (tiers.astype(f32) + 2.0) * (0.5 * LANES)
    distance = jnp.abs(index - halo - column).astype(f32) / radius
    return jnp.exp(-2.0 * distance * distance)


def sums_kernel(members, halo):
    def kernel(window_ref, lists_ref, tiers_ref, sums_ref, flat):
        for t in range(window_ref.shape[0]):
            raw = window_ref[t].astype(f32)
            observ = raw[:members]
            mean = jnp.sum(observ, axis=0, keepdims=True) * (1.0 / members)
            anomaly = observ - mean
            innov = raw[members : members + 1] - mean
            noise = raw[members + 1 : members + 2]
            energy = jnp.sum(anomaly * anomaly, axis=0, keepdims=True)
            flat[t, 0:SUB] = jnp.broadcast_to(innov * innov / noise, (SUB, LANES))
            flat[t, SUB : 2 * SUB] = jnp.broadcast_to(energy / noise, (SUB, LANES))

        def tile_sum(tile, carry):
            fit, spread = carry
            fit_rows = [flat[tile + t, 0:SUB] for t in range(SPAN)]
            spread_rows = [flat[tile + t, SUB : 2 * SUB] for t in range(SPAN)]
            for s in range(LANES // SUB):
                start = pl.multiple_of(tile * LANES + s * SUB, SUB)
                rows = pl.ds(start, SUB)
                index = lists_ref[rows, :]
                local = index - tile * LANES
                low, high = local & (LANES - 1), local >> 7
                decay = decay_of(index, start, tiers_ref[rows, :], halo)
                a = b = jnp.zeros((SUB, LANES), f32)
                for t in range(SPAN):
                    here = high == t
                    fits = jnp.take_along_axis(fit_rows[t], low, axis=1, mode="promise_in_bounds")
                    spreads = jnp.take_along_axis(spread_rows[t], low, axis=1, mode="promise_in_bounds")
                    a, b = jnp.where(here, fits, a), jnp.where(here, spreads, b)
                fit, spread = fit + decay * a, spread + decay * b
            return fit, spread

        zero = jnp.zeros((SUB, LANES), f32)
        fit, spread = lax.fori_loop(0, lists_ref.shape[0] // LANES, tile_sum, (zero, zero))
        sums_ref[0:1, :] = jnp.sum(fit, axis=0, keepdims=True)
        sums_ref[1:2, :] = jnp.sum(spread, axis=0, keepdims=True)

    return kernel


def block_sums(window, lists, tiers, members, halo):
    return pl.pallas_call(
        sums_kernel(members, halo),
        in_specs=[vmem()] * 3,
        out_specs=vmem(),
        out_shape=jax.ShapeDtypeStruct((2, LANES), f32),
        scratch_shapes=[pltpu.VMEM((window.shape[0], 2 * SUB, LANES), f32)],
        cost_estimate=pl.CostEstimate(flops=10_000_000, bytes_accessed=1_000_000, transcendentals=100_000),
        name="block_sums",
    )(window, lists, tiers)


def split(value):
    high = value.astype(bf16)
    return high, (value - high.astype(f32)).astype(bf16)


def gram_kernel(members, halo):
    def kernel(first_ref, window_ref, lists_ref, tiers_ref, gram_ref):
        def block(b, unused):
            rows = pl.ds(pl.multiple_of(b * SUB, SUB), SUB)
            start = first_ref[0] + b * SUB
            index = lists_ref[rows, :]
            decay = decay_of(index, start, tiers_ref[rows, :], halo)
            tile = start // LANES
            local = index - tile * LANES
            table = jnp.concatenate([window_ref[tile + t] for t in range(SPAN)], axis=1)
            place = lax.broadcasted_iota(jnp.int32, (SPAN * LANES, LANES), 0)
            for s in range(SUB):
                chosen = jnp.where(place == local[s : s + 1], 1.0, 0.0).astype(bf16)
                picked = jnp.dot(table, chosen, preferred_element_type=f32)
                mean = jnp.sum(picked[:members], axis=0, keepdims=True) * (1.0 / members)
                anomaly = picked - mean
                weight = decay[s : s + 1] / picked[members + 1 : members + 2]
                high, low = split(anomaly)
                weighted_high, weighted_low = split(anomaly[:members] * weight)
                left = jnp.concatenate([weighted_high, weighted_high, weighted_low], axis=1)
                right = jnp.concatenate([high, low, high], axis=1)
                gram_ref[b * SUB + s] = lax.dot_general(left, right, NT, preferred_element_type=f32)
            return unused

        lax.fori_loop(0, gram_ref.shape[0] // SUB, block, 0)

    return kernel


def grams(first, window, lists, tiers, members, halo):
    own = lists.shape[0]
    return pl.pallas_call(
        gram_kernel(members, halo),
        in_specs=[smem(), vmem(), vmem(), vmem()],
        out_specs=vmem(),
        out_shape=jax.ShapeDtypeStruct((own, members, members + SUB), f32),
        cost_estimate=pl.CostEstimate(flops=own * 60_000_000, bytes_accessed=own * 40_000, transcendentals=own * LANES),
        name="grams",
    )(first, window, lists, tiers)


def product(a, b):
    size = a.shape[0]
    pad = LANES - size
    (ah, al), (bh, bl) = split(a), split(b)
    wide, tall = jnp.zeros((size, pad), bf16), jnp.zeros((pad, size), bf16)
    left = jnp.concatenate([ah, wide, al, wide, ah, wide], axis=1)
    right = jnp.concatenate([bh, tall, bh, tall, bl, tall], axis=0)
    return jnp.dot(left, right, preferred_element_type=f32)


def root_kernel(members, parts):
    def kernel(mine_ref, other_ref, *refs):
        gram_refs, trans_ref = refs[:parts], refs[parts]
        total = mine_ref[...] + other_ref[...]
        ridge = jnp.sum(total[1:2], axis=1, keepdims=True) / jnp.sum(total[0:1], axis=1, keepdims=True)
        row = lax.broadcasted_iota(jnp.int32, (members, members), 0)
        col = lax.broadcasted_iota(jnp.int32, (members, members), 1)
        eye = jnp.where(row == col, 1.0, 0.0)
        offset = 0
        for gram_ref in gram_refs:
            own = gram_ref.shape[0]

            def block(b, unused, gram_ref=gram_ref, offset=offset):
                at = [b * BATCH + s for s in range(BATCH)]
                raw = [gram_ref[n] for n in at]
                mats = [r[:, :members] + ridge * eye for r in raw]
                bounds = [
                    jnp.max(jnp.sum(jnp.abs(m), axis=0, keepdims=True), axis=1, keepdims=True) for m in mats
                ]
                s0 = [m * (1.0 / bound) for m, bound in zip(mats, bounds)]
                q0 = [product(s, s) for s in s0]
                s1 = [2.25 * s + (product(q, 0.25 * s) - 1.5 * q) for s, q in zip(s0, q0)]
                q1 = [product(s, s) for s in s1]
                a = [0.25 * product(s, r) - 0.75 * (s + r) for s, r in zip(s0, s1)]
                s2 = [2.25 * s + (product(q, 0.25 * s) - 1.5 * q) for s, q in zip(s1, q1)]
                q2 = [product(s, s) for s in s2]
                c = [1.6875 * q - 2.4375 * s + product(q, 0.0625 * q - 0.5625 * s) for s, q in zip(s2, q2)]
                z = [5.0625 * eye + 2.25 * (x + y) + product(x, y) for x, y in zip(a, c)]
                root = [v / jnp.sqrt(bound) for v, bound in zip(z, bounds)]
                half = [jnp.sum(r * g[:, members : members + 1], axis=0, keepdims=True) for r, g in zip(root, raw)]
                gain = [jnp.sum(r * h, axis=1, keepdims=True) for r, h in zip(root, half)]
                for n, r, g in zip(at, root, gain):
                    full = r * ((members - 1.0) ** 0.5) + g
                    full = full - (jnp.sum(full, axis=0, keepdims=True) - 1.0) * (1.0 / members)
                    trans_ref[offset + n] = full.astype(bf16)
                return unused

            lax.fori_loop(0, own // BATCH, block, 0)
            offset += own

    return kernel


def roots(mine, other, pieces, members):
    own = sum(p.shape[0] for p in pieces)
    return pl.pallas_call(
        root_kernel(members, len(pieces)),
        in_specs=[vmem()] * (2 + len(pieces)),
        out_specs=vmem(),
        out_shape=jax.ShapeDtypeStruct((own, members, members), bf16),
        cost_estimate=pl.CostEstimate(flops=own * 60_000_000, bytes_accessed=own * 50_000, transcendentals=0),
        name="roots",
    )(mine, other, *pieces)


def per_device(
    prior_trials,
    prior_at_sensors,
    sensor_readings,
    sensor_noise_spread,
    nearby_readings,
    subarea_cutoff_level,
):
    held, patch_cells, quantities = prior_trials.shape
    obs_count = nearby_readings.shape[1]
    halo_cells = 5 * obs_count // 2
    groups = lax.axis_size(MEMBER)
    members = held * groups
    domains = patch_cells // groups

    gathered = spread_copies(prior_at_sensors, MEMBER).reshape(members, patch_cells)
    outgoing = prior_trials.reshape(held, groups, domains, quantities).transpose(1, 0, 2, 3)
    incoming = lax.all_to_all(outgoing, MEMBER, split_axis=0, concat_axis=0, tiled=True)
    incoming = incoming.reshape(members, domains, quantities)

    obs_rows = jnp.stack([sensor_readings, sensor_noise_spread], axis=0)
    window = with_halo(jnp.concatenate([gathered, obs_rows], axis=0), "space", halo_cells)
    tiles = patch_cells // LANES + SPAN
    window = jnp.pad(window, ((0, SUB - 2), (0, tiles * LANES - window.shape[1])))
    window = window.reshape(members + SUB, tiles, LANES).transpose(1, 0, 2)

    tiers = subarea_cutoff_level[:, None]
    first = (lax.axis_index(MEMBER) * domains).astype(jnp.int32)
    own_lists = lax.dynamic_slice_in_dim(nearby_readings, first, domains, 0)
    own_tiers = lax.dynamic_slice_in_dim(tiers, first, domains, 0)
    mine = block_sums(window, nearby_readings, tiers, members, halo_cells)
    share = domains // 3
    pieces = []
    for r in range(3):
        other = shifted(mine, "space", 1 << r)
        part = slice(r * share, (r + 1) * share)
        start = (first + r * share).reshape(1)
        pieces.append(grams(start, window, own_lists[part], own_tiers[part], members, halo_cells))
        if r < 2:
            mine = mine + other
    trans_w = roots(mine, other, pieces, members)

    updated = jnp.einsum("inc,nij->jnc", incoming, trans_w, preferred_element_type=f32).astype(bf16)
    returned = lax.all_to_all(
        updated.reshape(groups, held, domains, quantities), MEMBER, split_axis=0, concat_axis=0, tiled=True
    )
    return returned.transpose(1, 0, 2, 3).reshape(held, patch_cells, quantities)


def solution(mesh):
    finer = Mesh(
        mesh.devices.reshape(mesh.shape["region"], mesh.shape["member"] // 2, 2, mesh.shape["space"]),
        ("region", "member_0", "member_1", "space"),
    )
    return jax.shard_map(
        per_device,
        mesh=finer,
        in_specs=(
            P(MEMBER, ("region", "space"), None),
            P(MEMBER, ("region", "space")),
            P(("region", "space")),
            P(("region", "space")),
            P(("region", "space"), None),
            P(("region", "space")),
        ),
        out_specs=P(MEMBER, ("region", "space"), None),
        check_vma=False,
    )
```

```python
import jax
import jax.numpy as jnp
from jax import lax
from jax.experimental import pallas as pl
from jax.experimental.pallas import tpu as pltpu
from jax.sharding import Mesh
from jax.sharding import PartitionSpec as P


MEMBER = ("member_0", "member_1")
LANES = 128
SUB = 8
SPAN = 6
BATCH = 16
f32, bf16 = jnp.float32, jnp.bfloat16
NT = (((1,), (1,)), ((), ()))


def vmem():
    return pl.BlockSpec(memory_space=pltpu.VMEM)


def smem():
    return pl.BlockSpec(memory_space=pltpu.SMEM)


def spread_copies(value, axis):
    copies = jnp.broadcast_to(value, (lax.axis_size(axis), *value.shape))
    return lax.all_to_all(copies, axis, split_axis=0, concat_axis=0, tiled=True)


def shifted(value, axis, step):
    count = lax.axis_size(axis)
    return lax.ppermute(value, axis, [(i, (i + step) % count) for i in range(count)])


def with_halo(value, axis, width):
    count, length = lax.axis_size(axis), value.shape[1]
    up = [(i, i + 1) for i in range(count - 1)]
    down = [(j, i) for i, j in up]
    before = lax.ppermute(value[:, length - width :], axis, up)
    after = lax.ppermute(value[:, :width], axis, down)
    return jnp.concatenate([before, value, after], axis=1)


def sums_kernel(members, halo):
    def kernel(first_ref, tiers_ref, window_ref, lists_ref, sums_ref, local_ref, decay_ref, flat):
        sub = lax.broadcasted_iota(jnp.int32, (SUB, LANES), 0)

        def decay_at(index, start):
            tier = jnp.zeros((SUB, LANES), jnp.int32)
            for s in range(SUB):
                tier = jnp.where(sub == s, tiers_ref[start + s], tier)
            radius = (tier.astype(f32) + 2.0) * (0.5 * LANES)
            distance = jnp.abs(index - halo - start - sub).astype(f32) / radius
            return jnp.exp(-2.0 * distance * distance)

        for t in range(window_ref.shape[0]):
            raw = window_ref[t].astype(f32)
            observ = raw[:members]
            mean = jnp.sum(observ, axis=0, keepdims=True) * (1.0 / members)
            anomaly = observ - mean
            innov = raw[members : members + 1] - mean
            scale = 1.0 / raw[members + 1 : members + 2]
            energy = jnp.sum(anomaly * anomaly, axis=0, keepdims=True)
            flat[t, 0:SUB] = jnp.broadcast_to(innov * innov * scale, (SUB, LANES))
            flat[t, SUB : 2 * SUB] = jnp.broadcast_to(energy * scale, (SUB, LANES))

        def own_rows(b, unused):
            start = pl.multiple_of(first_ref[0] + b * SUB, SUB)
            rows = pl.ds(pl.multiple_of(b * SUB, SUB), SUB)
            index = lists_ref[pl.ds(start, SUB), :]
            local_ref[rows, :] = index - start // LANES * LANES
            decay_ref[rows, :] = decay_at(index, start)
            return unused

        lax.fori_loop(0, local_ref.shape[0] // SUB, own_rows, 0)

        def tile_sum(tile, carry):
            fit, spread = carry
            fit_rows = [flat[tile + t, 0:SUB] for t in range(SPAN)]
            spread_rows = [flat[tile + t, SUB : 2 * SUB] for t in range(SPAN)]
            for s in range(LANES // SUB):
                start = pl.multiple_of(tile * LANES + s * SUB, SUB)
                index = lists_ref[pl.ds(start, SUB), :]
                local = index - tile * LANES
                low, high = local & (LANES - 1), local >> 7
                decay = decay_at(index, start)
                a = b = jnp.zeros((SUB, LANES), f32)
                for t in range(SPAN):
                    here = high == t
                    fits = jnp.take_along_axis(fit_rows[t], low, axis=1, mode="promise_in_bounds")
                    spreads = jnp.take_along_axis(spread_rows[t], low, axis=1, mode="promise_in_bounds")
                    a, b = jnp.where(here, fits, a), jnp.where(here, spreads, b)
                fit, spread = fit + decay * a, spread + decay * b
            return fit, spread

        zero = jnp.zeros((SUB, LANES), f32)
        fit, spread = lax.fori_loop(0, lists_ref.shape[0] // LANES, tile_sum, (zero, zero))
        sums_ref[0:1, :] = jnp.sum(fit, axis=0, keepdims=True)
        sums_ref[1:2, :] = jnp.sum(spread, axis=0, keepdims=True)

    return kernel


def block_sums(first, tiers, window, lists, members, own, halo):
    return pl.pallas_call(
        sums_kernel(members, halo),
        in_specs=[smem(), smem(), vmem(), vmem()],
        out_specs=[vmem()] * 3,
        out_shape=[
            jax.ShapeDtypeStruct((2, LANES), f32),
            jax.ShapeDtypeStruct((own, LANES), jnp.int32),
            jax.ShapeDtypeStruct((own, LANES), f32),
        ],
        scratch_shapes=[pltpu.VMEM((window.shape[0], 2 * SUB, LANES), f32)],
        cost_estimate=pl.CostEstimate(flops=10_000_000, bytes_accessed=1_000_000, transcendentals=100_000),
        name="block_sums",
    )(first, tiers, window, lists)


def split(value):
    high = value.astype(bf16)
    return high, (value - high.astype(f32)).astype(bf16)


def gram_kernel(members, skip):
    def kernel(first_ref, window_ref, local_ref, decay_ref, gram_ref, place):
        place[...] = lax.broadcasted_iota(jnp.int32, (SPAN * LANES, LANES), 0)

        def block(b, unused):
            tile = (first_ref[0] + skip + b * SUB) // LANES
            rows = pl.ds(pl.multiple_of(b * SUB, SUB), SUB)
            local, decay = local_ref[rows, :], decay_ref[rows, :]
            table = jnp.concatenate([window_ref[tile + t] for t in range(SPAN)], axis=1)
            for s in range(0, SUB, 2):
                chosen = [jnp.where(place[...] == local[n : n + 1], 1.0, 0.0).astype(bf16) for n in (s, s + 1)]
                both = jnp.dot(table, jnp.concatenate(chosen, axis=1), preferred_element_type=f32)
                for i in range(2):
                    n = s + i
                    picked = both[:, i * LANES : (i + 1) * LANES]
                    mean = jnp.sum(picked[:members], axis=0, keepdims=True) * (1.0 / members)
                    anomaly = picked - mean
                    weight = decay[n : n + 1] / picked[members + 1 : members + 2]
                    high, low = split(anomaly)
                    weighted_high, weighted_low = split(anomaly[:members] * weight)
                    left = jnp.concatenate([weighted_high, weighted_high, weighted_low], axis=1)
                    right = jnp.concatenate([high, low, high], axis=1)
                    gram_ref[b * SUB + n] = lax.dot_general(left, right, NT, preferred_element_type=f32)
            return unused

        lax.fori_loop(0, gram_ref.shape[0] // SUB, block, 0)

    return kernel


def grams(first, window, local, decay, members, part, parts):
    own = local.shape[0] // parts
    return pl.pallas_call(
        gram_kernel(members, part * own),
        grid=(1,),
        in_specs=[
            smem(),
            pl.BlockSpec(window.shape, lambda i: (0, 0, 0)),
            pl.BlockSpec((own, LANES), lambda i: (part, 0)),
            pl.BlockSpec((own, LANES), lambda i: (part, 0)),
        ],
        out_specs=pl.BlockSpec((own, members, members + SUB), lambda i: (0, 0, 0)),
        out_shape=jax.ShapeDtypeStruct((own, members, members + SUB), f32),
        scratch_shapes=[pltpu.VMEM((SPAN * LANES, LANES), jnp.int32)],
        cost_estimate=pl.CostEstimate(flops=own * 60_000_000, bytes_accessed=own * 40_000, transcendentals=0),
        name="grams",
    )(first, window, local, decay)


def products(left, right):
    size = left[0].shape[0]
    gap = jnp.zeros((3 * size, LANES - size), bf16)
    results = []
    for i in range(0, len(left), 2):
        rows, columns = [], []
        for a, b in zip(left[i : i + 2], right[i : i + 2]):
            (ah, al), (bh, bl) = split(a), split(b)
            rows.append(jnp.concatenate([ah, al, ah], axis=1))
            columns += [jnp.concatenate([bh, bh, bl], axis=0), gap]
        both = jnp.dot(
            jnp.concatenate(rows, axis=0), jnp.concatenate(columns, axis=1), preferred_element_type=f32
        )
        results += [both[:size, :size], both[size:, LANES : LANES + size]]
    return results


def root_kernel(members, parts):
    def kernel(sums_ref, other_ref, *refs):
        gram_refs, trans_ref = refs[:parts], refs[parts]
        total = sums_ref[...] + other_ref[...]
        ridge = jnp.sum(total[1:2], axis=1, keepdims=True) / jnp.sum(total[0:1], axis=1, keepdims=True)
        row = lax.broadcasted_iota(jnp.int32, (members, members), 0)
        col = lax.broadcasted_iota(jnp.int32, (members, members), 1)
        eye = jnp.where(row == col, 1.0, 0.0)
        offset = 0
        for gram_ref in gram_refs:
            own = gram_ref.shape[0]

            def block(b, unused, gram_ref=gram_ref, offset=offset):
                at = [b * BATCH + s for s in range(BATCH)]
                raw = [gram_ref[n] for n in at]
                mats = [r[:, :members] + ridge * eye for r in raw]
                bounds = [
                    jnp.max(jnp.sum(jnp.abs(m), axis=0, keepdims=True), axis=1, keepdims=True) for m in mats
                ]
                s0 = [m * (1.0 / bound) for m, bound in zip(mats, bounds)]
                q0 = products(s0, s0)
                s1 = [2.25 * s + (x - 1.5 * q) for s, q, x in zip(s0, q0, products(q0, [0.25 * s for s in s0]))]
                q1 = products(s1, s1)
                a = [0.25 * x - 0.75 * (s + r) for s, r, x in zip(s0, s1, products(s0, s1))]
                s2 = [2.25 * s + (x - 1.5 * q) for s, q, x in zip(s1, q1, products(q1, [0.25 * s for s in s1]))]
                q2 = products(s2, s2)
                rest = products(q2, [0.0625 * q - 0.5625 * s for s, q in zip(s2, q2)])
                c = [1.6875 * q - 2.4375 * s + x for s, q, x in zip(s2, q2, rest)]
                z = [5.0625 * eye + 2.25 * (x + y) + w for x, y, w in zip(a, c, products(a, c))]
                root = [v / jnp.sqrt(bound) for v, bound in zip(z, bounds)]
                half = [jnp.sum(r * g[:, members : members + 1], axis=0, keepdims=True) for r, g in zip(root, raw)]
                gain = [jnp.sum(r * h, axis=1, keepdims=True) for r, h in zip(root, half)]
                for n, r, g in zip(at, root, gain):
                    full = r * ((members - 1.0) ** 0.5) + g
                    full = full - (jnp.sum(full, axis=0, keepdims=True) - 1.0) * (1.0 / members)
                    trans_ref[offset + n] = full.astype(bf16)
                return unused

            lax.fori_loop(0, own // BATCH, block, 0)
            offset += own

    return kernel


def roots(mine, other, pieces, members):
    own = sum(p.shape[0] for p in pieces)
    return pl.pallas_call(
        root_kernel(members, len(pieces)),
        in_specs=[vmem()] * (2 + len(pieces)),
        out_specs=vmem(),
        out_shape=jax.ShapeDtypeStruct((own, members, members), bf16),
        cost_estimate=pl.CostEstimate(flops=own * 60_000_000, bytes_accessed=own * 50_000, transcendentals=0),
        name="roots",
    )(mine, other, *pieces)


def per_device(
    prior_trials,
    prior_at_sensors,
    sensor_readings,
    sensor_noise_spread,
    nearby_readings,
    subarea_cutoff_level,
):
    held, patch_cells, quantities = prior_trials.shape
    obs_count = nearby_readings.shape[1]
    halo_cells = 5 * obs_count // 2
    groups = lax.axis_size(MEMBER)
    members = held * groups
    domains = patch_cells // groups

    gathered = spread_copies(prior_at_sensors, MEMBER).reshape(members, patch_cells)
    outgoing = prior_trials.reshape(held, groups, domains, quantities).transpose(1, 0, 2, 3)
    incoming = lax.all_to_all(outgoing, MEMBER, split_axis=0, concat_axis=0, tiled=True)
    incoming = incoming.reshape(members, domains, quantities)

    obs_rows = jnp.stack([sensor_readings, sensor_noise_spread], axis=0)
    window = with_halo(jnp.concatenate([gathered, obs_rows], axis=0), "space", halo_cells)
    tiles = patch_cells // LANES + SPAN
    window = jnp.pad(window, ((0, SUB - 2), (0, tiles * LANES - window.shape[1])))
    window = window.reshape(members + SUB, tiles, LANES).transpose(1, 0, 2)

    first = (lax.axis_index(MEMBER) * domains).astype(jnp.int32).reshape(1)
    mine, local, decay = block_sums(first, subarea_cutoff_level, window, nearby_readings, members, domains, halo_cells)
    pieces = []
    for r in range(3):
        other = shifted(mine, "space", 1 << r)
        pieces.append(grams(first, window, local, decay, members, r, 3))
        if r < 2:
            mine = mine + other
    trans_w = roots(mine, other, pieces, members)

    updated = jnp.einsum("inc,nij->jnc", incoming, trans_w, preferred_element_type=f32).astype(bf16)
    returned = lax.all_to_all(
        updated.reshape(groups, held, domains, quantities), MEMBER, split_axis=0, concat_axis=0, tiled=True
    )
    return returned.transpose(1, 0, 2, 3).reshape(held, patch_cells, quantities)


def solution(mesh):
    finer = Mesh(
        mesh.devices.reshape(mesh.shape["region"], mesh.shape["member"] // 2, 2, mesh.shape["space"]),
        ("region", "member_0", "member_1", "space"),
    )
    return jax.shard_map(
        per_device,
        mesh=finer,
        in_specs=(
            P(MEMBER, ("region", "space"), None),
            P(MEMBER, ("region", "space")),
            P(("region", "space")),
            P(("region", "space")),
            P(("region", "space"), None),
            P(("region", "space")),
        ),
        out_specs=P(MEMBER, ("region", "space"), None),
        check_vma=False,
    )
```

```python
import jax
import jax.numpy as jnp
from jax import lax
from jax.experimental import pallas as pl
from jax.experimental.pallas import tpu as pltpu
from jax.sharding import Mesh
from jax.sharding import PartitionSpec as P


MEMBER = ("member_0", "member_1")
LANES = 128
SUB = 8
SPAN = 6
BATCH = 16
f32, bf16 = jnp.float32, jnp.bfloat16
NT = (((1,), (1,)), ((), ()))


def vmem():
    return pl.BlockSpec(memory_space=pltpu.VMEM)


def smem():
    return pl.BlockSpec(memory_space=pltpu.SMEM)


def spread_copies(value, axis):
    copies = jnp.broadcast_to(value, (lax.axis_size(axis), *value.shape))
    return lax.all_to_all(copies, axis, split_axis=0, concat_axis=0, tiled=True)


def shifted(value, axis, step):
    count = lax.axis_size(axis)
    return lax.ppermute(value, axis, [(i, (i + step) % count) for i in range(count)])


def with_halo(value, axis, width):
    count, length = lax.axis_size(axis), value.shape[1]
    up = [(i, i + 1) for i in range(count - 1)]
    down = [(j, i) for i, j in up]
    before = lax.ppermute(value[:, length - width :], axis, up)
    after = lax.ppermute(value[:, :width], axis, down)
    return jnp.concatenate([before, value, after], axis=1)


def sums_kernel(members, halo):
    def kernel(first_ref, tiers_ref, window_ref, lists_ref, sums_ref, local_ref, decay_ref, flat):
        sub = lax.broadcasted_iota(jnp.int32, (SUB, LANES), 0)

        def decay_at(index, start):
            tier = jnp.zeros((SUB, LANES), jnp.int32)
            for s in range(SUB):
                tier = jnp.where(sub == s, tiers_ref[start + s], tier)
            radius = (tier.astype(f32) + 2.0) * (0.5 * LANES)
            distance = jnp.abs(index - halo - start - sub).astype(f32) / radius
            return jnp.exp(-2.0 * distance * distance)

        for t in range(window_ref.shape[0]):
            raw = window_ref[t].astype(f32)
            observ = raw[:members]
            mean = jnp.sum(observ, axis=0, keepdims=True) * (1.0 / members)
            anomaly = observ - mean
            innov = raw[members : members + 1] - mean
            scale = 1.0 / raw[members + 1 : members + 2]
            energy = jnp.sum(anomaly * anomaly, axis=0, keepdims=True)
            flat[t, 0:SUB] = jnp.broadcast_to(innov * innov * scale, (SUB, LANES))
            flat[t, SUB : 2 * SUB] = jnp.broadcast_to(energy * scale, (SUB, LANES))

        def own_rows(b, unused):
            start = pl.multiple_of(first_ref[0] + b * SUB, SUB)
            rows = pl.ds(pl.multiple_of(b * SUB, SUB), SUB)
            index = lists_ref[pl.ds(start, SUB), :]
            local_ref[rows, :] = index - start // LANES * LANES
            decay_ref[rows, :] = decay_at(index, start)
            return unused

        lax.fori_loop(0, local_ref.shape[0] // SUB, own_rows, 0)

        def tile_sum(tile, carry):
            fit, spread = carry
            fit_rows = [flat[tile + t, 0:SUB] for t in range(SPAN)]
            spread_rows = [flat[tile + t, SUB : 2 * SUB] for t in range(SPAN)]
            for s in range(LANES // SUB):
                start = pl.multiple_of(tile * LANES + s * SUB, SUB)
                index = lists_ref[pl.ds(start, SUB), :]
                local = index - tile * LANES
                low, high = local & (LANES - 1), local >> 7
                decay = decay_at(index, start)
                a = b = jnp.zeros((SUB, LANES), f32)
                for t in range(SPAN):
                    here = high == t
                    fits = jnp.take_along_axis(fit_rows[t], low, axis=1, mode="promise_in_bounds")
                    spreads = jnp.take_along_axis(spread_rows[t], low, axis=1, mode="promise_in_bounds")
                    a, b = jnp.where(here, fits, a), jnp.where(here, spreads, b)
                fit, spread = fit + decay * a, spread + decay * b
            return fit, spread

        zero = jnp.zeros((SUB, LANES), f32)
        fit, spread = lax.fori_loop(0, lists_ref.shape[0] // LANES, tile_sum, (zero, zero))
        sums_ref[0:1, :] = jnp.sum(fit, axis=0, keepdims=True)
        sums_ref[1:2, :] = jnp.sum(spread, axis=0, keepdims=True)

    return kernel


def block_sums(first, tiers, window, lists, members, own, halo):
    return pl.pallas_call(
        sums_kernel(members, halo),
        in_specs=[smem(), smem(), vmem(), vmem()],
        out_specs=[vmem()] * 3,
        out_shape=[
            jax.ShapeDtypeStruct((2, LANES), f32),
            jax.ShapeDtypeStruct((own, LANES), jnp.int32),
            jax.ShapeDtypeStruct((own, LANES), f32),
        ],
        scratch_shapes=[pltpu.VMEM((window.shape[0], 2 * SUB, LANES), f32)],
        cost_estimate=pl.CostEstimate(flops=10_000_000, bytes_accessed=1_000_000, transcendentals=100_000),
        name="block_sums",
    )(first, tiers, window, lists)


def split(value):
    high = value.astype(bf16)
    return high, (value - high.astype(f32)).astype(bf16)


def gram_kernel(members, skip):
    def kernel(first_ref, window_ref, local_ref, decay_ref, gram_ref, place):
        place[...] = lax.broadcasted_iota(jnp.int32, (SPAN * LANES, LANES), 0)

        def block(b, unused):
            tile = (first_ref[0] + skip + b * SUB) // LANES
            rows = pl.ds(pl.multiple_of(b * SUB, SUB), SUB)
            local, decay = local_ref[rows, :], decay_ref[rows, :]
            table = jnp.concatenate([window_ref[tile + t] for t in range(SPAN)], axis=1)
            for s in range(0, SUB, 2):
                chosen = [jnp.where(place[...] == local[n : n + 1], 1.0, 0.0).astype(bf16) for n in (s, s + 1)]
                both = jnp.dot(table, jnp.concatenate(chosen, axis=1), preferred_element_type=f32)
                for i in range(2):
                    n = s + i
                    picked = both[:, i * LANES : (i + 1) * LANES]
                    mean = jnp.sum(picked[:members], axis=0, keepdims=True) * (1.0 / members)
                    anomaly = picked - mean
                    weight = decay[n : n + 1] / picked[members + 1 : members + 2]
                    high, low = split(anomaly)
                    weighted_high, weighted_low = split(anomaly[:members] * weight)
                    left = jnp.concatenate([weighted_high, weighted_high, weighted_low], axis=1)
                    right = jnp.concatenate([high, low, high], axis=1)
                    gram_ref[b * SUB + n] = lax.dot_general(left, right, NT, preferred_element_type=f32)
            return unused

        lax.fori_loop(0, gram_ref.shape[0] // SUB, block, 0)

    return kernel


def grams(first, window, local, decay, members, part, parts):
    own = local.shape[0] // parts
    return pl.pallas_call(
        gram_kernel(members, part * own),
        grid=(1,),
        in_specs=[
            smem(),
            pl.BlockSpec(window.shape, lambda i: (0, 0, 0)),
            pl.BlockSpec((own, LANES), lambda i: (part, 0)),
            pl.BlockSpec((own, LANES), lambda i: (part, 0)),
        ],
        out_specs=pl.BlockSpec((own, members, members + SUB), lambda i: (0, 0, 0)),
        out_shape=jax.ShapeDtypeStruct((own, members, members + SUB), f32),
        scratch_shapes=[pltpu.VMEM((SPAN * LANES, LANES), jnp.int32)],
        cost_estimate=pl.CostEstimate(flops=own * 60_000_000, bytes_accessed=own * 40_000, transcendentals=0),
        name="grams",
    )(first, window, local, decay)


def products(left, right):
    size = left[0].shape[0]
    gap = jnp.zeros((3 * size, LANES - size), bf16)
    results = []
    for i in range(0, len(left), 2):
        rows, columns = [], []
        for a, b in zip(left[i : i + 2], right[i : i + 2]):
            (ah, al), (bh, bl) = split(a), split(b)
            rows.append(jnp.concatenate([ah, al, ah], axis=1))
            columns += [jnp.concatenate([bh, bh, bl], axis=0), gap]
        both = jnp.dot(
            jnp.concatenate(rows, axis=0), jnp.concatenate(columns, axis=1), preferred_element_type=f32
        )
        results += [both[:size, :size], both[size:, LANES : LANES + size]]
    return results


def root_kernel(members, parts):
    def kernel(sums_ref, other_ref, *refs):
        gram_refs, trans_ref = refs[:parts], refs[parts]
        total = sums_ref[...] + other_ref[...]
        ridge = jnp.sum(total[1:2], axis=1, keepdims=True) / jnp.sum(total[0:1], axis=1, keepdims=True)
        row = lax.broadcasted_iota(jnp.int32, (members, members), 0)
        col = lax.broadcasted_iota(jnp.int32, (members, members), 1)
        eye = jnp.where(row == col, 1.0, 0.0)
        offset = 0
        for gram_ref in gram_refs:
            own = gram_ref.shape[0]

            def block(b, unused, gram_ref=gram_ref, offset=offset):
                at = [b * BATCH + s for s in range(BATCH)]
                raw = [gram_ref[n] for n in at]
                mats = [r[:, :members] + ridge * eye for r in raw]
                bounds = [
                    jnp.max(jnp.sum(jnp.abs(m), axis=0, keepdims=True), axis=1, keepdims=True) for m in mats
                ]
                s0 = [m * (1.0 / bound) for m, bound in zip(mats, bounds)]
                q0 = products(s0, s0)
                s1 = [2.25 * s + (x - 1.5 * q) for s, q, x in zip(s0, q0, products(q0, [0.25 * s for s in s0]))]
                q1 = products(s1, s1)
                a = [0.25 * x - 0.75 * (s + r) for s, r, x in zip(s0, s1, products(s0, s1))]
                s2 = [2.25 * s + (x - 1.5 * q) for s, q, x in zip(s1, q1, products(q1, [0.25 * s for s in s1]))]
                q2 = products(s2, s2)
                rest = products(q2, [0.0625 * q - 0.5625 * s for s, q in zip(s2, q2)])
                c = [1.6875 * q - 2.4375 * s + x for s, q, x in zip(s2, q2, rest)]
                z = [5.0625 * eye + 2.25 * (x + y) + w for x, y, w in zip(a, c, products(a, c))]
                root = [v / jnp.sqrt(bound) for v, bound in zip(z, bounds)]
                half = [jnp.sum(r * g[:, members : members + 1], axis=0, keepdims=True) for r, g in zip(root, raw)]
                gain = [jnp.sum(r * h, axis=1, keepdims=True) for r, h in zip(root, half)]
                for n, r, g in zip(at, root, gain):
                    full = r * ((members - 1.0) ** 0.5) + g
                    full = full - (jnp.sum(full, axis=0, keepdims=True) - 1.0) * (1.0 / members)
                    trans_ref[offset + n] = full.astype(bf16)
                return unused

            lax.fori_loop(0, own // BATCH, block, 0)
            offset += own

    return kernel


def roots(mine, other, pieces, members):
    own = sum(p.shape[0] for p in pieces)
    return pl.pallas_call(
        root_kernel(members, len(pieces)),
        in_specs=[vmem()] * (2 + len(pieces)),
        out_specs=vmem(),
        out_shape=jax.ShapeDtypeStruct((own, members, members), bf16),
        cost_estimate=pl.CostEstimate(flops=own * 60_000_000, bytes_accessed=own * 50_000, transcendentals=0),
        name="roots",
    )(mine, other, *pieces)


def per_device(
    prior_trials,
    prior_at_sensors,
    sensor_readings,
    sensor_noise_spread,
    nearby_readings,
    subarea_cutoff_level,
):
    held, patch_cells, quantities = prior_trials.shape
    obs_count = nearby_readings.shape[1]
    halo_cells = 5 * obs_count // 2
    groups = lax.axis_size(MEMBER)
    members = held * groups
    domains = patch_cells // groups

    chunks = patch_cells // LANES
    dense = prior_at_sensors.reshape(held, chunks, LANES).transpose(1, 0, 2).reshape(-1, LANES)
    lines = dense.shape[0]
    dense = jnp.pad(dense, ((0, -lines % (2 * SUB)), (0, 0)))
    gathered = spread_copies(dense, MEMBER).reshape(groups, -1, LANES)[:, :lines]
    gathered = gathered.reshape(groups, chunks, held, LANES).transpose(0, 2, 1, 3).reshape(members, patch_cells)
    outgoing = prior_trials.reshape(held, groups, domains, quantities).transpose(1, 0, 2, 3)
    incoming = lax.all_to_all(outgoing, MEMBER, split_axis=0, concat_axis=0, tiled=True)
    incoming = incoming.reshape(members, domains, quantities)

    obs_rows = jnp.stack([sensor_readings, sensor_noise_spread], axis=0)
    window = with_halo(jnp.concatenate([gathered, obs_rows], axis=0), "space", halo_cells)
    tiles = patch_cells // LANES + SPAN
    window = jnp.pad(window, ((0, SUB - 2), (0, tiles * LANES - window.shape[1])))
    window = window.reshape(members + SUB, tiles, LANES).transpose(1, 0, 2)

    first = (lax.axis_index(MEMBER) * domains).astype(jnp.int32).reshape(1)
    mine, local, decay = block_sums(first, subarea_cutoff_level, window, nearby_readings, members, domains, halo_cells)
    pieces = []
    for r in range(3):
        other = shifted(mine, "space", 1 << r)
        pieces.append(grams(first, window, local, decay, members, r, 3))
        if r < 2:
            mine = mine + other
    trans_w = roots(mine, other, pieces, members)

    updated = jnp.einsum("inc,nij->jnc", incoming, trans_w, preferred_element_type=f32).astype(bf16)
    returned = lax.all_to_all(
        updated.reshape(groups, held, domains, quantities), MEMBER, split_axis=0, concat_axis=0, tiled=True
    )
    return returned.transpose(1, 0, 2, 3).reshape(held, patch_cells, quantities)


def solution(mesh):
    finer = Mesh(
        mesh.devices.reshape(mesh.shape["region"], mesh.shape["member"] // 2, 2, mesh.shape["space"]),
        ("region", "member_0", "member_1", "space"),
    )
    return jax.shard_map(
        per_device,
        mesh=finer,
        in_specs=(
            P(MEMBER, ("region", "space"), None),
            P(MEMBER, ("region", "space")),
            P(("region", "space")),
            P(("region", "space")),
            P(("region", "space"), None),
            P(("region", "space")),
        ),
        out_specs=P(MEMBER, ("region", "space"), None),
        check_vma=False,
    )
```

```python
import jax
import jax.numpy as jnp
from jax import lax
from jax.experimental import pallas as pl
from jax.experimental.pallas import tpu as pltpu
from jax.sharding import Mesh
from jax.sharding import PartitionSpec as P


MEMBER = ("member_0", "member_1")
LANES = 128
SUB = 8
SPAN = 6
BATCH = 16
LATE = 6
f32, bf16 = jnp.float32, jnp.bfloat16
NT = (((1,), (1,)), ((), ()))


def vmem():
    return pl.BlockSpec(memory_space=pltpu.VMEM)


def smem():
    return pl.BlockSpec(memory_space=pltpu.SMEM)


def spread_copies(value, axis):
    copies = jnp.broadcast_to(value, (lax.axis_size(axis), *value.shape))
    return lax.all_to_all(copies, axis, split_axis=0, concat_axis=0, tiled=True)


def shifted(value, axis, step):
    count = lax.axis_size(axis)
    return lax.ppermute(value, axis, [(i, (i + step) % count) for i in range(count)])


def with_halo(value, axis, width):
    count, length = lax.axis_size(axis), value.shape[1]
    up = [(i, i + 1) for i in range(count - 1)]
    down = [(j, i) for i, j in up]
    before = lax.ppermute(value[:, length - width :], axis, up)
    after = lax.ppermute(value[:, :width], axis, down)
    return jnp.concatenate([before, value, after], axis=1)


def sums_kernel(members, halo):
    def kernel(first_ref, tiers_ref, window_ref, lists_ref, sums_ref, local_ref, decay_ref, flat):
        sub = lax.broadcasted_iota(jnp.int32, (SUB, LANES), 0)

        def decay_at(index, start):
            tier = jnp.zeros((SUB, LANES), jnp.int32)
            for s in range(SUB):
                tier = jnp.where(sub == s, tiers_ref[start + s], tier)
            radius = (tier.astype(f32) + 2.0) * (0.5 * LANES)
            distance = jnp.abs(index - halo - start - sub).astype(f32) / radius
            return jnp.exp(-2.0 * distance * distance)

        for t in range(window_ref.shape[0]):
            raw = window_ref[t].astype(f32)
            observ = raw[:members]
            mean = jnp.sum(observ, axis=0, keepdims=True) * (1.0 / members)
            anomaly = observ - mean
            innov = raw[members : members + 1] - mean
            scale = 1.0 / raw[members + 1 : members + 2]
            energy = jnp.sum(anomaly * anomaly, axis=0, keepdims=True)
            flat[t, 0:SUB] = jnp.broadcast_to(innov * innov * scale, (SUB, LANES))
            flat[t, SUB : 2 * SUB] = jnp.broadcast_to(energy * scale, (SUB, LANES))

        def own_rows(b, unused):
            start = pl.multiple_of(first_ref[0] + b * SUB, SUB)
            rows = pl.ds(pl.multiple_of(b * SUB, SUB), SUB)
            index = lists_ref[pl.ds(start, SUB), :]
            local_ref[rows, :] = index - start // LANES * LANES
            decay_ref[rows, :] = decay_at(index, start)
            return unused

        lax.fori_loop(0, local_ref.shape[0] // SUB, own_rows, 0)

        def tile_sum(tile, carry):
            fit, spread = carry
            fit_rows = [flat[tile + t, 0:SUB] for t in range(SPAN)]
            spread_rows = [flat[tile + t, SUB : 2 * SUB] for t in range(SPAN)]
            for s in range(LANES // SUB):
                start = pl.multiple_of(tile * LANES + s * SUB, SUB)
                index = lists_ref[pl.ds(start, SUB), :]
                local = index - tile * LANES
                low, high = local & (LANES - 1), local >> 7
                decay = decay_at(index, start)
                a = b = jnp.zeros((SUB, LANES), f32)
                for t in range(SPAN):
                    here = high == t
                    fits = jnp.take_along_axis(fit_rows[t], low, axis=1, mode="promise_in_bounds")
                    spreads = jnp.take_along_axis(spread_rows[t], low, axis=1, mode="promise_in_bounds")
                    a, b = jnp.where(here, fits, a), jnp.where(here, spreads, b)
                fit, spread = fit + decay * a, spread + decay * b
            return fit, spread

        zero = jnp.zeros((SUB, LANES), f32)
        fit, spread = lax.fori_loop(0, lists_ref.shape[0] // LANES, tile_sum, (zero, zero))
        sums_ref[0:1, :] = jnp.sum(fit, axis=0, keepdims=True)
        sums_ref[1:2, :] = jnp.sum(spread, axis=0, keepdims=True)

    return kernel


def block_sums(first, tiers, window, lists, members, own, halo):
    return pl.pallas_call(
        sums_kernel(members, halo),
        in_specs=[smem(), smem(), vmem(), vmem()],
        out_specs=[vmem()] * 3,
        out_shape=[
            jax.ShapeDtypeStruct((2, LANES), f32),
            jax.ShapeDtypeStruct((own, LANES), jnp.int32),
            jax.ShapeDtypeStruct((own, LANES), f32),
        ],
        scratch_shapes=[pltpu.VMEM((window.shape[0], 2 * SUB, LANES), f32)],
        cost_estimate=pl.CostEstimate(flops=10_000_000, bytes_accessed=1_000_000, transcendentals=100_000),
        name="block_sums",
    )(first, tiers, window, lists)


def split(value):
    high = value.astype(bf16)
    return high, (value - high.astype(f32)).astype(bf16)


def gram_kernel(members, skip):
    def kernel(first_ref, window_ref, local_ref, decay_ref, gram_ref, place):
        place[...] = lax.broadcasted_iota(jnp.int32, (SPAN * LANES, LANES), 0)

        def block(b, unused):
            tile = (first_ref[0] + skip + b * SUB) // LANES
            rows = pl.ds(pl.multiple_of(b * SUB, SUB), SUB)
            local, decay = local_ref[rows, :], decay_ref[rows, :]
            table = jnp.concatenate([window_ref[tile + t] for t in range(SPAN)], axis=1)
            for s in range(0, SUB, 2):
                chosen = [jnp.where(place[...] == local[n : n + 1], 1.0, 0.0).astype(bf16) for n in (s, s + 1)]
                both = jnp.dot(table, jnp.concatenate(chosen, axis=1), preferred_element_type=f32)
                for i in range(2):
                    n = s + i
                    picked = both[:, i * LANES : (i + 1) * LANES]
                    mean = jnp.sum(picked[:members], axis=0, keepdims=True) * (1.0 / members)
                    anomaly = picked - mean
                    weight = decay[n : n + 1] / picked[members + 1 : members + 2]
                    high, low = split(anomaly)
                    weighted_high, weighted_low = split(anomaly[:members] * weight)
                    left = jnp.concatenate([weighted_high, weighted_high, weighted_low], axis=1)
                    right = jnp.concatenate([high, low, high], axis=1)
                    gram_ref[b * SUB + n] = lax.dot_general(left, right, NT, preferred_element_type=f32)
            return unused

        lax.fori_loop(0, gram_ref.shape[0] // SUB, block, 0)

    return kernel


def grams(first, window, local, decay, members, part, parts):
    own = local.shape[0] // parts
    return pl.pallas_call(
        gram_kernel(members, part * own),
        grid=(1,),
        in_specs=[
            smem(),
            pl.BlockSpec(window.shape, lambda i: (0, 0, 0)),
            pl.BlockSpec((own, LANES), lambda i: (part, 0)),
            pl.BlockSpec((own, LANES), lambda i: (part, 0)),
        ],
        out_specs=pl.BlockSpec((own, members, members + SUB), lambda i: (0, 0, 0)),
        out_shape=jax.ShapeDtypeStruct((own, members, members + SUB), f32),
        scratch_shapes=[pltpu.VMEM((SPAN * LANES, LANES), jnp.int32)],
        cost_estimate=pl.CostEstimate(flops=own * 60_000_000, bytes_accessed=own * 40_000, transcendentals=0),
        name="grams",
    )(first, window, local, decay)


def products(left, right):
    size = left[0].shape[0]
    gap = jnp.zeros((3 * size, LANES - size), bf16)
    results = []
    for i in range(0, len(left), 2):
        rows, columns = [], []
        for a, b in zip(left[i : i + 2], right[i : i + 2]):
            (ah, al), (bh, bl) = split(a), split(b)
            rows.append(jnp.concatenate([ah, al, ah], axis=1))
            columns += [jnp.concatenate([bh, bh, bl], axis=0), gap]
        both = jnp.dot(
            jnp.concatenate(rows, axis=0), jnp.concatenate(columns, axis=1), preferred_element_type=f32
        )
        results += [both[:size, :size], both[size:, LANES : LANES + size]]
    return results


def root_kernel(members, parts):
    def kernel(sums_ref, other_ref, order_ref, *refs):
        gram_refs, trans_ref = refs[:parts], refs[parts]
        order = order_ref[...]
        total = sums_ref[...] + other_ref[...]
        ridge = jnp.sum(total[1:2], axis=1, keepdims=True) / jnp.sum(total[0:1], axis=1, keepdims=True)
        row = lax.broadcasted_iota(jnp.int32, (members, members), 0)
        col = lax.broadcasted_iota(jnp.int32, (members, members), 1)
        eye = jnp.where(row == col, 1.0, 0.0)
        offset = 0
        for gram_ref in gram_refs:
            own = gram_ref.shape[0]

            def block(b, unused, gram_ref=gram_ref, offset=offset):
                at = [b * BATCH + s for s in range(BATCH)]
                raw = [gram_ref[n] for n in at]
                mats = [r[:, :members] + ridge * eye for r in raw]
                bounds = [
                    jnp.max(jnp.sum(jnp.abs(m), axis=0, keepdims=True), axis=1, keepdims=True) for m in mats
                ]
                s0 = [m * (1.0 / bound) for m, bound in zip(mats, bounds)]
                q0 = products(s0, s0)
                s1 = [2.25 * s + (x - 1.5 * q) for s, q, x in zip(s0, q0, products(q0, [0.25 * s for s in s0]))]
                q1 = products(s1, s1)
                a = [0.25 * x - 0.75 * (s + r) for s, r, x in zip(s0, s1, products(s0, s1))]
                s2 = [2.25 * s + (x - 1.5 * q) for s, q, x in zip(s1, q1, products(q1, [0.25 * s for s in s1]))]
                q2 = products(s2, s2)
                rest = products(q2, [0.0625 * q - 0.5625 * s for s, q in zip(s2, q2)])
                c = [1.6875 * q - 2.4375 * s + x for s, q, x in zip(s2, q2, rest)]
                z = [5.0625 * eye + 2.25 * (x + y) + w for x, y, w in zip(a, c, products(a, c))]
                root = [v / jnp.sqrt(bound) for v, bound in zip(z, bounds)]
                half = [jnp.sum(r * g[:, members : members + 1], axis=0, keepdims=True) for r, g in zip(root, raw)]
                gain = [jnp.sum(r * h, axis=1, keepdims=True) for r, h in zip(root, half)]
                for n, r, g in zip(at, root, gain):
                    full = r * ((members - 1.0) ** 0.5) + g
                    full = full - (jnp.sum(full, axis=0, keepdims=True) - 1.0) * (1.0 / members)
                    turned = jnp.dot(full.astype(bf16), order, preferred_element_type=f32)
                    trans_ref[offset + n] = turned.astype(bf16)
                return unused

            lax.fori_loop(0, own // BATCH, block, 0)
            offset += own

    return kernel


def roots(mine, other, order, pieces, members):
    own = sum(p.shape[0] for p in pieces)
    return pl.pallas_call(
        root_kernel(members, len(pieces)),
        in_specs=[vmem()] * (3 + len(pieces)),
        out_specs=vmem(),
        out_shape=jax.ShapeDtypeStruct((own, members, members), bf16),
        cost_estimate=pl.CostEstimate(flops=own * 60_000_000, bytes_accessed=own * 50_000, transcendentals=0),
        name="roots",
    )(mine, other, order, *pieces)


def place_kernel(skip, count):
    def kernel(starts_ref, *refs):
        block_refs, (out_ref, sems) = refs[:count], refs[-2:]
        width = block_refs[0].shape[1]
        copies = []
        for k, ref in enumerate(block_refs):
            columns = pl.ds(pl.multiple_of(starts_ref[skip + k], SUB), width)
            copies.append(pltpu.make_async_copy(ref, out_ref.at[:, columns, :], sems.at[k]))
            copies[-1].start()
        for copy in copies:
            copy.wait()

    return kernel


def place(starts, blocks, skip, size, into=()):
    held, _, quantities = blocks[0].shape
    anywhere = pl.BlockSpec(memory_space=pl.ANY)
    count = len(blocks)
    return pl.pallas_call(
        place_kernel(skip, count),
        in_specs=[smem()] + [vmem()] * count + [anywhere] * len(into),
        out_specs=anywhere,
        out_shape=jax.ShapeDtypeStruct((held, size, quantities), blocks[0].dtype),
        scratch_shapes=[pltpu.SemaphoreType.DMA((count,))],
        input_output_aliases={1 + count: 0} if into else {},
        cost_estimate=pl.CostEstimate(flops=1_000_000, bytes_accessed=count * 300_000, transcendentals=0),
        name="place",
    )(starts, *blocks, *into)


def routes(chips):
    steps = []
    for far in range(chips // 2, 0, -1):
        steps += [far] if 2 * far == chips else [far, -far]
    return [(0, 0)] + [(step, flip) for step in steps for flip in (0, 1)] + [(0, 1)]


def sent(value, step, flip):
    chips = lax.axis_size(MEMBER[0])
    pairs = [
        (2 * chip + core, 2 * ((chip + step) % chips) + (core ^ flip)) for chip in range(chips) for core in (0, 1)
    ]
    return lax.ppermute(value, MEMBER, pairs)


def per_device(
    prior_trials,
    prior_at_sensors,
    sensor_readings,
    sensor_noise_spread,
    nearby_readings,
    subarea_cutoff_level,
):
    held, patch_cells, quantities = prior_trials.shape
    obs_count = nearby_readings.shape[1]
    halo_cells = 5 * obs_count // 2
    groups = lax.axis_size(MEMBER)
    members = held * groups
    domains = patch_cells // groups

    chunks = patch_cells // LANES
    dense = prior_at_sensors.reshape(held, chunks, LANES).transpose(1, 0, 2).reshape(-1, LANES)
    lines = dense.shape[0]
    dense = jnp.pad(dense, ((0, -lines % (2 * SUB)), (0, 0)))
    gathered = spread_copies(dense, MEMBER).reshape(groups, -1, LANES)[:, :lines]
    gathered = gathered.reshape(groups, chunks, held, LANES).transpose(0, 2, 1, 3).reshape(members, patch_cells)
    outgoing = prior_trials.reshape(held, groups, domains, quantities).transpose(1, 0, 2, 3)
    incoming = lax.all_to_all(outgoing, MEMBER, split_axis=0, concat_axis=0, tiled=True)
    incoming = incoming.reshape(members, domains, quantities)

    obs_rows = jnp.stack([sensor_readings, sensor_noise_spread], axis=0)
    window = with_halo(jnp.concatenate([gathered, obs_rows], axis=0), "space", halo_cells)
    tiles = patch_cells // LANES + SPAN
    window = jnp.pad(window, ((0, SUB - 2), (0, tiles * LANES - window.shape[1])))
    window = window.reshape(members + SUB, tiles, LANES).transpose(1, 0, 2)

    first = (lax.axis_index(MEMBER) * domains).astype(jnp.int32).reshape(1)
    mine, local, decay = block_sums(first, subarea_cutoff_level, window, nearby_readings, members, domains, halo_cells)
    pieces = []
    for r in range(3):
        other = shifted(mine, "space", 1 << r)
        pieces.append(grams(first, window, local, decay, members, r, 3))
        if r < 2:
            mine = mine + other
    row, core = (lax.axis_index(name) for name in MEMBER)
    chips = lax.axis_size(MEMBER[0])
    paths = routes(chips)
    steps, flips = (jnp.array(values, jnp.int32) for values in zip(*paths))
    target = 2 * lax.rem(row + steps + chips, chips) + lax.rem(core + flips, 2)
    source = 2 * lax.rem(row - steps + chips, chips) + lax.rem(core + flips, 2)
    member = jnp.arange(members, dtype=jnp.int32)
    wanted = (target[:, None] * held + jnp.arange(held, dtype=jnp.int32)[None]).reshape(members)
    order = (member[:, None] == wanted[None]).astype(bf16)
    trans_w = roots(mine, other, order, pieces, members)

    updated = jnp.einsum("inc,nij->jnc", incoming, trans_w, preferred_element_type=f32).astype(bf16)
    slots = updated.reshape(groups, held, domains, quantities)
    arrived = [slots[0]]
    for k, (step, flip) in enumerate(paths[1:], 1):
        arrived.append(sent(slots[k], step, flip))
    starts = source * domains
    early = len(arrived) - LATE
    result = place(starts, arrived[:early], 0, patch_cells)
    return place(starts, arrived[early:], early, patch_cells, (result,))


def solution(mesh):
    finer = Mesh(
        mesh.devices.reshape(mesh.shape["region"], mesh.shape["member"] // 2, 2, mesh.shape["space"]),
        ("region", "member_0", "member_1", "space"),
    )
    return jax.shard_map(
        per_device,
        mesh=finer,
        in_specs=(
            P(MEMBER, ("region", "space"), None),
            P(MEMBER, ("region", "space")),
            P(("region", "space")),
            P(("region", "space")),
            P(("region", "space"), None),
            P(("region", "space")),
        ),
        out_specs=P(MEMBER, ("region", "space"), None),
        check_vma=False,
    )
```

```python
import jax
import jax.numpy as jnp
from jax import lax
from jax.experimental import pallas as pl
from jax.experimental.pallas import tpu as pltpu
from jax.sharding import Mesh
from jax.sharding import PartitionSpec as P


MEMBER = ("member_0", "member_1")
LANES = 128
SUB = 8
SPAN = 6
BATCH = 16
LATE = 6
f32, bf16 = jnp.float32, jnp.bfloat16
NT = (((1,), (1,)), ((), ()))


def vmem():
    return pl.BlockSpec(memory_space=pltpu.VMEM)


def smem():
    return pl.BlockSpec(memory_space=pltpu.SMEM)


def spread_copies(value, axis):
    copies = jnp.broadcast_to(value, (lax.axis_size(axis), *value.shape))
    return lax.all_to_all(copies, axis, split_axis=0, concat_axis=0, tiled=True)


def shifted(value, axis, step):
    count = lax.axis_size(axis)
    return lax.ppermute(value, axis, [(i, (i + step) % count) for i in range(count)])


def with_halo(value, axis, width):
    count, length = lax.axis_size(axis), value.shape[1]
    up = [(i, i + 1) for i in range(count - 1)]
    down = [(j, i) for i, j in up]
    before = lax.ppermute(value[:, length - width :], axis, up)
    after = lax.ppermute(value[:, :width], axis, down)
    return jnp.concatenate([before, value, after], axis=1)


def sums_kernel(members, halo):
    def kernel(first_ref, tiers_ref, window_ref, lists_ref, sums_ref, local_ref, decay_ref, flat):
        sub = lax.broadcasted_iota(jnp.int32, (SUB, LANES), 0)

        def decay_at(index, start):
            tier = jnp.zeros((SUB, LANES), jnp.int32)
            for s in range(SUB):
                tier = jnp.where(sub == s, tiers_ref[start + s], tier)
            radius = (tier.astype(f32) + 2.0) * (0.5 * LANES)
            distance = jnp.abs(index - halo - start - sub).astype(f32) / radius
            return jnp.exp(-2.0 * distance * distance)

        for t in range(window_ref.shape[0]):
            raw = window_ref[t].astype(f32)
            observ = raw[:members]
            mean = jnp.sum(observ, axis=0, keepdims=True) * (1.0 / members)
            anomaly = observ - mean
            innov = raw[members : members + 1] - mean
            scale = 1.0 / raw[members + 1 : members + 2]
            energy = jnp.sum(anomaly * anomaly, axis=0, keepdims=True)
            flat[t, 0:SUB] = jnp.broadcast_to(innov * innov * scale, (SUB, LANES))
            flat[t, SUB : 2 * SUB] = jnp.broadcast_to(energy * scale, (SUB, LANES))

        def own_rows(b, unused):
            start = pl.multiple_of(first_ref[0] + b * SUB, SUB)
            rows = pl.ds(pl.multiple_of(b * SUB, SUB), SUB)
            index = lists_ref[pl.ds(start, SUB), :]
            local_ref[rows, :] = index - start // LANES * LANES
            decay_ref[rows, :] = decay_at(index, start)
            return unused

        lax.fori_loop(0, local_ref.shape[0] // SUB, own_rows, 0)

        def tile_sum(tile, carry):
            fit, spread = carry
            fit_rows = [flat[tile + t, 0:SUB] for t in range(SPAN)]
            spread_rows = [flat[tile + t, SUB : 2 * SUB] for t in range(SPAN)]
            for s in range(LANES // SUB):
                start = pl.multiple_of(tile * LANES + s * SUB, SUB)
                index = lists_ref[pl.ds(start, SUB), :]
                local = index - tile * LANES
                low, high = local & (LANES - 1), local >> 7
                decay = decay_at(index, start)
                a = b = jnp.zeros((SUB, LANES), f32)
                for t in range(SPAN):
                    here = high == t
                    fits = jnp.take_along_axis(fit_rows[t], low, axis=1, mode="promise_in_bounds")
                    spreads = jnp.take_along_axis(spread_rows[t], low, axis=1, mode="promise_in_bounds")
                    a, b = jnp.where(here, fits, a), jnp.where(here, spreads, b)
                fit, spread = fit + decay * a, spread + decay * b
            return fit, spread

        zero = jnp.zeros((SUB, LANES), f32)
        fit, spread = lax.fori_loop(0, lists_ref.shape[0] // LANES, tile_sum, (zero, zero))
        sums_ref[0:1, :] = jnp.sum(fit, axis=0, keepdims=True)
        sums_ref[1:2, :] = jnp.sum(spread, axis=0, keepdims=True)

    return kernel


def block_sums(first, tiers, window, lists, members, own, halo):
    return pl.pallas_call(
        sums_kernel(members, halo),
        in_specs=[smem(), smem(), vmem(), vmem()],
        out_specs=[vmem()] * 3,
        out_shape=[
            jax.ShapeDtypeStruct((2, LANES), f32),
            jax.ShapeDtypeStruct((own, LANES), jnp.int32),
            jax.ShapeDtypeStruct((own, LANES), f32),
        ],
        scratch_shapes=[pltpu.VMEM((window.shape[0], 2 * SUB, LANES), f32)],
        cost_estimate=pl.CostEstimate(flops=10_000_000, bytes_accessed=1_000_000, transcendentals=100_000),
        name="block_sums",
    )(first, tiers, window, lists)


def split(value):
    high = value.astype(bf16)
    return high, (value - high.astype(f32)).astype(bf16)


def gram_kernel(members, skip):
    def kernel(first_ref, window_ref, local_ref, decay_ref, gram_ref, place):
        place[...] = lax.broadcasted_iota(jnp.int32, (SPAN * LANES, LANES), 0)

        def block(b, unused):
            tile = (first_ref[0] + skip + b * SUB) // LANES
            rows = pl.ds(pl.multiple_of(b * SUB, SUB), SUB)
            local, decay = local_ref[rows, :], decay_ref[rows, :]
            table = jnp.concatenate([window_ref[tile + t] for t in range(SPAN)], axis=1)
            for s in range(0, SUB, 2):
                chosen = [jnp.where(place[...] == local[n : n + 1], 1.0, 0.0).astype(bf16) for n in (s, s + 1)]
                both = jnp.dot(table, jnp.concatenate(chosen, axis=1), preferred_element_type=f32)
                for i in range(2):
                    n = s + i
                    picked = both[:, i * LANES : (i + 1) * LANES]
                    mean = jnp.sum(picked[:members], axis=0, keepdims=True) * (1.0 / members)
                    anomaly = picked - mean
                    weight = decay[n : n + 1] / picked[members + 1 : members + 2]
                    high, low = split(anomaly)
                    weighted_high, weighted_low = split(anomaly[:members] * weight)
                    left = jnp.concatenate([weighted_high, weighted_high, weighted_low], axis=1)
                    right = jnp.concatenate([high, low, high], axis=1)
                    gram_ref[b * SUB + n] = lax.dot_general(left, right, NT, preferred_element_type=f32)
            return unused

        lax.fori_loop(0, gram_ref.shape[0] // SUB, block, 0)

    return kernel


def grams(first, window, local, decay, members, part, parts):
    own = local.shape[0] // parts
    return pl.pallas_call(
        gram_kernel(members, part * own),
        grid=(1,),
        in_specs=[
            smem(),
            pl.BlockSpec(window.shape, lambda i: (0, 0, 0)),
            pl.BlockSpec((own, LANES), lambda i: (part, 0)),
            pl.BlockSpec((own, LANES), lambda i: (part, 0)),
        ],
        out_specs=pl.BlockSpec((own, members, members + SUB), lambda i: (0, 0, 0)),
        out_shape=jax.ShapeDtypeStruct((own, members, members + SUB), f32),
        scratch_shapes=[pltpu.VMEM((SPAN * LANES, LANES), jnp.int32)],
        cost_estimate=pl.CostEstimate(flops=own * 60_000_000, bytes_accessed=own * 40_000, transcendentals=0),
        name="grams",
    )(first, window, local, decay)


def products(left, right):
    size = left[0].shape[0]
    gap = jnp.zeros((3 * size, LANES - size), bf16)
    results = []
    for i in range(0, len(left), 2):
        rows, columns = [], []
        for a, b in zip(left[i : i + 2], right[i : i + 2]):
            (ah, al), (bh, bl) = split(a), split(b)
            rows.append(jnp.concatenate([ah, al, ah], axis=1))
            columns += [jnp.concatenate([bh, bh, bl], axis=0), gap]
        both = jnp.dot(
            jnp.concatenate(rows, axis=0), jnp.concatenate(columns, axis=1), preferred_element_type=f32
        )
        results += [both[:size, :size], both[size:, LANES : LANES + size]]
    return results


def root_kernel(members, parts):
    def kernel(sums_ref, other_ref, order_ref, *refs):
        gram_refs, trans_ref = refs[:parts], refs[parts]
        order = order_ref[...]
        total = sums_ref[...] + other_ref[...]
        ridge = jnp.sum(total[1:2], axis=1, keepdims=True) / jnp.sum(total[0:1], axis=1, keepdims=True)
        row = lax.broadcasted_iota(jnp.int32, (members, members), 0)
        col = lax.broadcasted_iota(jnp.int32, (members, members), 1)
        eye = jnp.where(row == col, 1.0, 0.0)
        offset = 0
        for gram_ref in gram_refs:
            own = gram_ref.shape[0]

            def block(b, unused, gram_ref=gram_ref, offset=offset):
                at = [b * BATCH + s for s in range(BATCH)]
                raw = [gram_ref[n] for n in at]
                mats = [r[:, :members] + ridge * eye for r in raw]
                bounds = [
                    jnp.max(jnp.sum(jnp.abs(m), axis=0, keepdims=True), axis=1, keepdims=True) for m in mats
                ]
                s0 = [m * (1.0 / bound) for m, bound in zip(mats, bounds)]
                q0 = products(s0, s0)
                s1 = [2.25 * s + (x - 1.5 * q) for s, q, x in zip(s0, q0, products(q0, [0.25 * s for s in s0]))]
                q1 = products(s1, s1)
                a = [0.25 * x - 0.75 * (s + r) for s, r, x in zip(s0, s1, products(s0, s1))]
                s2 = [2.25 * s + (x - 1.5 * q) for s, q, x in zip(s1, q1, products(q1, [0.25 * s for s in s1]))]
                q2 = products(s2, s2)
                rest = products(q2, [0.0625 * q - 0.5625 * s for s, q in zip(s2, q2)])
                c = [1.6875 * q - 2.4375 * s + x for s, q, x in zip(s2, q2, rest)]
                z = [5.0625 * eye + 2.25 * (x + y) + w for x, y, w in zip(a, c, products(a, c))]
                root = [v / jnp.sqrt(bound) for v, bound in zip(z, bounds)]
                half = [jnp.sum(r * g[:, members : members + 1], axis=0, keepdims=True) for r, g in zip(root, raw)]
                gain = [jnp.sum(r * h, axis=1, keepdims=True) for r, h in zip(root, half)]
                for n, r, g in zip(at, root, gain):
                    full = r * ((members - 1.0) ** 0.5) + g
                    full = full - (jnp.sum(full, axis=0, keepdims=True) - 1.0) * (1.0 / members)
                    turned = jnp.dot(full.astype(bf16), order, preferred_element_type=f32)
                    trans_ref[offset + n] = turned.astype(bf16)
                return unused

            lax.fori_loop(0, own // BATCH, block, 0)
            offset += own

    return kernel


def roots(mine, other, order, pieces, members):
    own = sum(p.shape[0] for p in pieces)
    return pl.pallas_call(
        root_kernel(members, len(pieces)),
        in_specs=[vmem()] * (3 + len(pieces)),
        out_specs=vmem(),
        out_shape=jax.ShapeDtypeStruct((own, members, members), bf16),
        cost_estimate=pl.CostEstimate(flops=own * 60_000_000, bytes_accessed=own * 50_000, transcendentals=0),
        name="roots",
    )(mine, other, order, *pieces)


def place_kernel(skip, count):
    def kernel(starts_ref, *refs):
        block_refs, (out_ref, sems) = refs[:count], refs[-2:]
        width = block_refs[0].shape[1]
        copies = []
        for k, ref in enumerate(block_refs):
            columns = pl.ds(pl.multiple_of(starts_ref[skip + k], SUB), width)
            copies.append(pltpu.make_async_copy(ref, out_ref.at[:, columns, :], sems.at[k]))
            copies[-1].start()
        for copy in copies:
            copy.wait()

    return kernel


def place(starts, blocks, skip, size, into=()):
    held, _, quantities = blocks[0].shape
    anywhere = pl.BlockSpec(memory_space=pl.ANY)
    count = len(blocks)
    return pl.pallas_call(
        place_kernel(skip, count),
        in_specs=[smem()] + [vmem()] * count + [anywhere] * len(into),
        out_specs=anywhere,
        out_shape=jax.ShapeDtypeStruct((held, size, quantities), blocks[0].dtype),
        scratch_shapes=[pltpu.SemaphoreType.DMA((count,))],
        input_output_aliases={1 + count: 0} if into else {},
        cost_estimate=pl.CostEstimate(flops=1_000_000, bytes_accessed=count * 300_000, transcendentals=0),
        name="place",
    )(starts, *blocks, *into)


def routes(chips):
    steps = []
    for far in range(chips // 2, 0, -1):
        steps += [far] if 2 * far == chips else [far, -far]
    return [(0, 0)] + [(step, flip) for step in steps for flip in (0, 1)] + [(0, 1)]


def sent(value, step, flip):
    chips = lax.axis_size(MEMBER[0])
    pairs = [
        (2 * chip + core, 2 * ((chip + step) % chips) + (core ^ flip)) for chip in range(chips) for core in (0, 1)
    ]
    return lax.ppermute(value, MEMBER, pairs)


def per_device(
    prior_trials,
    prior_at_sensors,
    sensor_readings,
    sensor_noise_spread,
    nearby_readings,
    subarea_cutoff_level,
):
    held, patch_cells, quantities = prior_trials.shape
    obs_count = nearby_readings.shape[1]
    halo_cells = 5 * obs_count // 2
    groups = lax.axis_size(MEMBER)
    members = held * groups
    domains = patch_cells // groups

    chunks = patch_cells // LANES
    dense = prior_at_sensors.reshape(held, chunks, LANES).transpose(1, 0, 2).reshape(-1, LANES)
    lines = dense.shape[0]
    dense = jnp.pad(dense, ((0, -lines % (2 * SUB)), (0, 0)))
    gathered = spread_copies(dense, MEMBER).reshape(groups, -1, LANES)[:, :lines]
    gathered = gathered.reshape(groups, chunks, held, LANES).transpose(0, 2, 1, 3).reshape(members, patch_cells)
    outgoing = prior_trials.reshape(held, groups, domains, quantities).transpose(1, 0, 2, 3)
    incoming = lax.all_to_all(outgoing, MEMBER, split_axis=0, concat_axis=0, tiled=True)
    incoming = incoming.reshape(members, domains, quantities)

    obs_rows = jnp.stack([sensor_readings, sensor_noise_spread], axis=0)
    window = with_halo(jnp.concatenate([gathered, obs_rows], axis=0), "space", halo_cells)
    tiles = patch_cells // LANES + SPAN
    window = jnp.pad(window, ((0, SUB - 2), (0, tiles * LANES - window.shape[1])))
    window = window.reshape(members + SUB, tiles, LANES).transpose(1, 0, 2)

    first = (lax.axis_index(MEMBER) * domains).astype(jnp.int32).reshape(1)
    mine, local, decay = block_sums(first, subarea_cutoff_level, window, nearby_readings, members, domains, halo_cells)
    pieces = []
    for r in range(3):
        other = shifted(mine, "space", 1 << r)
        pieces.append(grams(first, window, local, decay, members, r, 3))
        if r < 2:
            mine = mine + other
    row, core = (lax.axis_index(name) for name in MEMBER)
    chips = lax.axis_size(MEMBER[0])
    paths = routes(chips)
    steps, flips = (jnp.array(values, jnp.int32) for values in zip(*paths))
    target = 2 * lax.rem(row + steps + chips, chips) + lax.rem(core + flips, 2)
    source = 2 * lax.rem(row - steps + chips, chips) + lax.rem(core + flips, 2)
    member = jnp.arange(members, dtype=jnp.int32)
    wanted = (target[:, None] * held + jnp.arange(held, dtype=jnp.int32)[None]).reshape(members)
    order = (member[:, None] == wanted[None]).astype(bf16)
    trans_w = roots(mine, other, order, pieces, members)

    def mixed(low, high):
        part = trans_w[:, :, low * held : high * held]
        part = jnp.einsum("inc,nij->jnc", incoming, part, preferred_element_type=f32).astype(bf16)
        return list(part.reshape(high - low, held, domains, quantities))

    slots = mixed(0, 3)
    slots = slots + mixed(3, groups)
    arrived = [slots[0]]
    for k, (step, flip) in enumerate(paths[1:], 1):
        arrived.append(sent(slots[k], step, flip))
    starts = source * domains
    early = len(arrived) - LATE
    result = place(starts, arrived[:early], 0, patch_cells)
    return place(starts, arrived[early:], early, patch_cells, (result,))


def solution(mesh):
    finer = Mesh(
        mesh.devices.reshape(mesh.shape["region"], mesh.shape["member"] // 2, 2, mesh.shape["space"]),
        ("region", "member_0", "member_1", "space"),
    )
    return jax.shard_map(
        per_device,
        mesh=finer,
        in_specs=(
            P(MEMBER, ("region", "space"), None),
            P(MEMBER, ("region", "space")),
            P(("region", "space")),
            P(("region", "space")),
            P(("region", "space"), None),
            P(("region", "space")),
        ),
        out_specs=P(MEMBER, ("region", "space"), None),
        check_vma=False,
    )
```

```python
import jax
import jax.numpy as jnp
from jax import lax
from jax.experimental import pallas as pl
from jax.experimental.pallas import tpu as pltpu
from jax.sharding import Mesh
from jax.sharding import PartitionSpec as P


MEMBER = ("member_0", "member_1")
LANES = 128
SUB = 8
SPAN = 6
BATCH = 16
LATE = 6
f32, bf16 = jnp.float32, jnp.bfloat16
NT = (((1,), (1,)), ((), ()))


def vmem():
    return pl.BlockSpec(memory_space=pltpu.VMEM)


def smem():
    return pl.BlockSpec(memory_space=pltpu.SMEM)


def spread_copies(value, axis):
    copies = jnp.broadcast_to(value, (lax.axis_size(axis), *value.shape))
    return lax.all_to_all(copies, axis, split_axis=0, concat_axis=0, tiled=True)


def shifted(value, axis, step):
    count = lax.axis_size(axis)
    return lax.ppermute(value, axis, [(i, (i + step) % count) for i in range(count)])


def with_halo(value, axis, width):
    count, length = lax.axis_size(axis), value.shape[1]
    up = [(i, i + 1) for i in range(count - 1)]
    down = [(j, i) for i, j in up]
    before = lax.ppermute(value[:, length - width :], axis, up)
    after = lax.ppermute(value[:, :width], axis, down)
    return jnp.concatenate([before, value, after], axis=1)


def sums_kernel(members, halo):
    def kernel(first_ref, tiers_ref, window_ref, lists_ref, sums_ref, local_ref, decay_ref, flat):
        sub = lax.broadcasted_iota(jnp.int32, (SUB, LANES), 0)

        def decay_at(index, start):
            tier = jnp.zeros((SUB, LANES), jnp.int32)
            for s in range(SUB):
                tier = jnp.where(sub == s, tiers_ref[start + s], tier)
            radius = (tier.astype(f32) + 2.0) * (0.5 * LANES)
            distance = jnp.abs(index - halo - start - sub).astype(f32) / radius
            return jnp.exp(-2.0 * distance * distance)

        for t in range(window_ref.shape[0]):
            raw = window_ref[t].astype(f32)
            observ = raw[:members]
            mean = jnp.sum(observ, axis=0, keepdims=True) * (1.0 / members)
            anomaly = observ - mean
            innov = raw[members : members + 1] - mean
            scale = 1.0 / raw[members + 1 : members + 2]
            energy = jnp.sum(anomaly * anomaly, axis=0, keepdims=True)
            flat[t, 0:SUB] = jnp.broadcast_to(innov * innov * scale, (SUB, LANES))
            flat[t, SUB : 2 * SUB] = jnp.broadcast_to(energy * scale, (SUB, LANES))

        def own_rows(b, unused):
            start = pl.multiple_of(first_ref[0] + b * SUB, SUB)
            rows = pl.ds(pl.multiple_of(b * SUB, SUB), SUB)
            index = lists_ref[pl.ds(start, SUB), :]
            local_ref[rows, :] = index - start // LANES * LANES
            decay_ref[rows, :] = decay_at(index, start)
            return unused

        lax.fori_loop(0, local_ref.shape[0] // SUB, own_rows, 0)

        def tile_sum(tile, carry):
            fit, spread = carry
            fit_rows = [flat[tile + t, 0:SUB] for t in range(SPAN)]
            spread_rows = [flat[tile + t, SUB : 2 * SUB] for t in range(SPAN)]
            for s in range(LANES // SUB):
                start = pl.multiple_of(tile * LANES + s * SUB, SUB)
                index = lists_ref[pl.ds(start, SUB), :]
                local = index - tile * LANES
                low, high = local & (LANES - 1), local >> 7
                decay = decay_at(index, start)
                a = b = jnp.zeros((SUB, LANES), f32)
                for t in range(SPAN):
                    here = high == t
                    fits = jnp.take_along_axis(fit_rows[t], low, axis=1, mode="promise_in_bounds")
                    spreads = jnp.take_along_axis(spread_rows[t], low, axis=1, mode="promise_in_bounds")
                    a, b = jnp.where(here, fits, a), jnp.where(here, spreads, b)
                fit, spread = fit + decay * a, spread + decay * b
            return fit, spread

        zero = jnp.zeros((SUB, LANES), f32)
        fit, spread = lax.fori_loop(0, lists_ref.shape[0] // LANES, tile_sum, (zero, zero))
        sums_ref[0:1, :] = jnp.sum(fit, axis=0, keepdims=True)
        sums_ref[1:2, :] = jnp.sum(spread, axis=0, keepdims=True)

    return kernel


def block_sums(first, tiers, window, lists, members, own, halo):
    return pl.pallas_call(
        sums_kernel(members, halo),
        in_specs=[smem(), smem(), vmem(), vmem()],
        out_specs=[vmem()] * 3,
        out_shape=[
            jax.ShapeDtypeStruct((2, LANES), f32),
            jax.ShapeDtypeStruct((own, LANES), jnp.int32),
            jax.ShapeDtypeStruct((own, LANES), f32),
        ],
        scratch_shapes=[pltpu.VMEM((window.shape[0], 2 * SUB, LANES), f32)],
        cost_estimate=pl.CostEstimate(flops=10_000_000, bytes_accessed=1_000_000, transcendentals=100_000),
        name="block_sums",
    )(first, tiers, window, lists)


def split(value):
    high = value.astype(bf16)
    return high, (value - high.astype(f32)).astype(bf16)


def gram_kernel(members, skip):
    def kernel(first_ref, window_ref, local_ref, decay_ref, gram_ref, place):
        place[...] = lax.broadcasted_iota(jnp.int32, (SPAN * LANES, LANES), 0)

        def block(b, unused):
            tile = (first_ref[0] + skip + b * SUB) // LANES
            rows = pl.ds(pl.multiple_of(b * SUB, SUB), SUB)
            local, decay = local_ref[rows, :], decay_ref[rows, :]
            table = jnp.concatenate([window_ref[tile + t] for t in range(SPAN)], axis=1)
            for s in range(0, SUB, 2):
                chosen = [jnp.where(place[...] == local[n : n + 1], 1.0, 0.0).astype(bf16) for n in (s, s + 1)]
                both = jnp.dot(table, jnp.concatenate(chosen, axis=1), preferred_element_type=f32)
                for i in range(2):
                    n = s + i
                    picked = both[:, i * LANES : (i + 1) * LANES]
                    mean = jnp.sum(picked[:members], axis=0, keepdims=True) * (1.0 / members)
                    anomaly = picked - mean
                    weight = decay[n : n + 1] / picked[members + 1 : members + 2]
                    high, low = split(anomaly)
                    weighted_high, weighted_low = split(anomaly[:members] * weight)
                    left = jnp.concatenate([weighted_high, weighted_high, weighted_low], axis=1)
                    right = jnp.concatenate([high, low, high], axis=1)
                    gram_ref[b * SUB + n] = lax.dot_general(left, right, NT, preferred_element_type=f32)
            return unused

        lax.fori_loop(0, gram_ref.shape[0] // SUB, block, 0)

    return kernel


def grams(first, window, local, decay, members, part, parts):
    own = local.shape[0] // parts
    return pl.pallas_call(
        gram_kernel(members, part * own),
        grid=(1,),
        in_specs=[
            smem(),
            pl.BlockSpec(window.shape, lambda i: (0, 0, 0)),
            pl.BlockSpec((own, LANES), lambda i: (part, 0)),
            pl.BlockSpec((own, LANES), lambda i: (part, 0)),
        ],
        out_specs=pl.BlockSpec((own, members, members + SUB), lambda i: (0, 0, 0)),
        out_shape=jax.ShapeDtypeStruct((own, members, members + SUB), f32),
        scratch_shapes=[pltpu.VMEM((SPAN * LANES, LANES), jnp.int32)],
        cost_estimate=pl.CostEstimate(flops=own * 60_000_000, bytes_accessed=own * 40_000, transcendentals=0),
        name="grams",
    )(first, window, local, decay)


def products(left, right):
    size = left[0].shape[0]
    gap = jnp.zeros((3 * size, LANES - size), bf16)
    results = []
    for i in range(0, len(left), 2):
        rows, columns = [], []
        for a, b in zip(left[i : i + 2], right[i : i + 2]):
            (ah, al), (bh, bl) = split(a), split(b)
            rows.append(jnp.concatenate([ah, al, ah], axis=1))
            columns += [jnp.concatenate([bh, bh, bl], axis=0), gap]
        both = jnp.dot(
            jnp.concatenate(rows, axis=0), jnp.concatenate(columns, axis=1), preferred_element_type=f32
        )
        results += [both[:size, :size], both[size:, LANES : LANES + size]]
    return results


def root_kernel(members, parts):
    def kernel(sums_ref, other_ref, order_ref, *refs):
        gram_refs, trans_ref = refs[:parts], refs[parts]
        order = order_ref[...]
        total = sums_ref[...] + other_ref[...]
        ridge = jnp.sum(total[1:2], axis=1, keepdims=True) / jnp.sum(total[0:1], axis=1, keepdims=True)
        row = lax.broadcasted_iota(jnp.int32, (members, members), 0)
        col = lax.broadcasted_iota(jnp.int32, (members, members), 1)
        eye = jnp.where(row == col, 1.0, 0.0)
        offset = 0
        for gram_ref in gram_refs:
            own = gram_ref.shape[0]

            def block(b, unused, gram_ref=gram_ref, offset=offset):
                at = [b * BATCH + s for s in range(BATCH)]
                raw = [gram_ref[n] for n in at]
                mats = [r[:, :members] + ridge * eye for r in raw]
                bounds = [
                    jnp.max(jnp.sum(jnp.abs(m), axis=0, keepdims=True), axis=1, keepdims=True) for m in mats
                ]
                s0 = [m * (1.0 / bound) for m, bound in zip(mats, bounds)]
                q0 = products(s0, s0)
                s1 = [2.25 * s + (x - 1.5 * q) for s, q, x in zip(s0, q0, products(q0, [0.25 * s for s in s0]))]
                q1 = products(s1, s1)
                a = [0.25 * x - 0.75 * (s + r) for s, r, x in zip(s0, s1, products(s0, s1))]
                s2 = [2.25 * s + (x - 1.5 * q) for s, q, x in zip(s1, q1, products(q1, [0.25 * s for s in s1]))]
                q2 = products(s2, s2)
                rest = products(q2, [0.0625 * q - 0.5625 * s for s, q in zip(s2, q2)])
                c = [1.6875 * q - 2.4375 * s + x for s, q, x in zip(s2, q2, rest)]
                z = [5.0625 * eye + 2.25 * (x + y) + w for x, y, w in zip(a, c, products(a, c))]
                root = [v / jnp.sqrt(bound) for v, bound in zip(z, bounds)]
                half = [jnp.sum(r * g[:, members : members + 1], axis=0, keepdims=True) for r, g in zip(root, raw)]
                gain = [jnp.sum(r * h, axis=1, keepdims=True) for r, h in zip(root, half)]
                for n, r, g in zip(at, root, gain):
                    full = r * ((members - 1.0) ** 0.5) + g
                    full = full - (jnp.sum(full, axis=0, keepdims=True) - 1.0) * (1.0 / members)
                    turned = jnp.dot(full.astype(bf16), order, preferred_element_type=f32)
                    trans_ref[offset + n] = turned.astype(bf16)
                return unused

            lax.fori_loop(0, own // BATCH, block, 0)
            offset += own

    return kernel


def roots(mine, other, order, pieces, members):
    own = sum(p.shape[0] for p in pieces)
    return pl.pallas_call(
        root_kernel(members, len(pieces)),
        in_specs=[vmem()] * (3 + len(pieces)),
        out_specs=vmem(),
        out_shape=jax.ShapeDtypeStruct((own, members, members), bf16),
        cost_estimate=pl.CostEstimate(flops=own * 60_000_000, bytes_accessed=own * 50_000, transcendentals=0),
        name="roots",
    )(mine, other, order, *pieces)


def place_kernel(skip, count):
    def kernel(starts_ref, *refs):
        block_refs, (out_ref, sems) = refs[:count], refs[-2:]
        width = block_refs[0].shape[1]
        copies = []
        for k, ref in enumerate(block_refs):
            columns = pl.ds(pl.multiple_of(starts_ref[skip + k], SUB), width)
            copies.append(pltpu.make_async_copy(ref, out_ref.at[:, columns, :], sems.at[k]))
            copies[-1].start()
        for copy in copies:
            copy.wait()

    return kernel


def place(starts, blocks, skip, size, into=()):
    held, _, quantities = blocks[0].shape
    anywhere = pl.BlockSpec(memory_space=pl.ANY)
    count = len(blocks)
    return pl.pallas_call(
        place_kernel(skip, count),
        in_specs=[smem()] + [vmem()] * count + [anywhere] * len(into),
        out_specs=anywhere,
        out_shape=jax.ShapeDtypeStruct((held, size, quantities), blocks[0].dtype),
        scratch_shapes=[pltpu.SemaphoreType.DMA((count,))],
        input_output_aliases={1 + count: 0} if into else {},
        cost_estimate=pl.CostEstimate(flops=1_000_000, bytes_accessed=count * 300_000, transcendentals=0),
        name="place",
    )(starts, *blocks, *into)


def routes(chips):
    others = []
    for far in range(chips // 2, 0, -1):
        ways = [far] if 2 * far == chips else [far, -far]
        others += [(step, flip) for flip in (0, 1) for step in ways]
    return [(0, 0)] + others + [(0, 1)]


def sent(value, step, flip):
    chips = lax.axis_size(MEMBER[0])
    pairs = [
        (2 * chip + core, 2 * ((chip + step) % chips) + (core ^ flip)) for chip in range(chips) for core in (0, 1)
    ]
    return lax.ppermute(value, MEMBER, pairs)


def per_device(
    prior_trials,
    prior_at_sensors,
    sensor_readings,
    sensor_noise_spread,
    nearby_readings,
    subarea_cutoff_level,
):
    held, patch_cells, quantities = prior_trials.shape
    obs_count = nearby_readings.shape[1]
    halo_cells = 5 * obs_count // 2
    groups = lax.axis_size(MEMBER)
    members = held * groups
    domains = patch_cells // groups

    chunks = patch_cells // LANES
    dense = prior_at_sensors.reshape(held, chunks, LANES).transpose(1, 0, 2).reshape(-1, LANES)
    lines = dense.shape[0]
    dense = jnp.pad(dense, ((0, -lines % (2 * SUB)), (0, 0)))
    gathered = spread_copies(dense, MEMBER).reshape(groups, -1, LANES)[:, :lines]
    gathered = gathered.reshape(groups, chunks, held, LANES).transpose(0, 2, 1, 3).reshape(members, patch_cells)
    outgoing = prior_trials.reshape(held, groups, domains, quantities).transpose(1, 0, 2, 3)
    incoming = lax.all_to_all(outgoing, MEMBER, split_axis=0, concat_axis=0, tiled=True)
    incoming = incoming.reshape(members, domains, quantities)

    obs_rows = jnp.stack([sensor_readings, sensor_noise_spread], axis=0)
    window = with_halo(jnp.concatenate([gathered, obs_rows], axis=0), "space", halo_cells)
    tiles = patch_cells // LANES + SPAN
    window = jnp.pad(window, ((0, SUB - 2), (0, tiles * LANES - window.shape[1])))
    window = window.reshape(members + SUB, tiles, LANES).transpose(1, 0, 2)

    first = (lax.axis_index(MEMBER) * domains).astype(jnp.int32).reshape(1)
    mine, local, decay = block_sums(first, subarea_cutoff_level, window, nearby_readings, members, domains, halo_cells)
    pieces = []
    for r in range(3):
        other = shifted(mine, "space", 1 << r)
        pieces.append(grams(first, window, local, decay, members, r, 3))
        if r < 2:
            mine = mine + other
    row, core = (lax.axis_index(name) for name in MEMBER)
    chips = lax.axis_size(MEMBER[0])
    paths = routes(chips)
    steps, flips = (jnp.array(values, jnp.int32) for values in zip(*paths))
    target = 2 * lax.rem(row + steps + chips, chips) + lax.rem(core + flips, 2)
    source = 2 * lax.rem(row - steps + chips, chips) + lax.rem(core + flips, 2)
    member = jnp.arange(members, dtype=jnp.int32)
    wanted = (target[:, None] * held + jnp.arange(held, dtype=jnp.int32)[None]).reshape(members)
    order = (member[:, None] == wanted[None]).astype(bf16)
    trans_w = roots(mine, other, order, pieces, members)

    updated = jnp.einsum("inc,nij->jnc", incoming, trans_w, preferred_element_type=f32).astype(bf16)
    slots = updated.reshape(groups, held, domains, quantities)
    arrived = [slots[0]]
    for k, (step, flip) in enumerate(paths[1:], 1):
        arrived.append(sent(slots[k], step, flip))
    starts = source * domains
    early = len(arrived) - LATE
    result = place(starts, arrived[:early], 0, patch_cells)
    return place(starts, arrived[early:], early, patch_cells, (result,))


def solution(mesh):
    finer = Mesh(
        mesh.devices.reshape(mesh.shape["region"], mesh.shape["member"] // 2, 2, mesh.shape["space"]),
        ("region", "member_0", "member_1", "space"),
    )
    return jax.shard_map(
        per_device,
        mesh=finer,
        in_specs=(
            P(MEMBER, ("region", "space"), None),
            P(MEMBER, ("region", "space")),
            P(("region", "space")),
            P(("region", "space")),
            P(("region", "space"), None),
            P(("region", "space")),
        ),
        out_specs=P(MEMBER, ("region", "space"), None),
        check_vma=False,
    )
```
